32 devices in a mesh: chan: 16 (over z, y, core), tm: 2 (over x).
Axes of the slice: x: 2, y: 2, z: 4, core: 2. Of those that a mesh axis runs over, the one named last changes fastest.
Arguments:
- voltages: bfloat16 [2, 512, 256, 512], P(None, None, 'chan', 'tm'), may hold values from -6 to 6, as said below
- flag_mask: int32 [4, 256], P('tm', 'chan'), may hold values from 0 to 1, as said below
- flagged_prefix_counts: int32 [4, 256], P('tm', 'chan'), may hold values from 0 to 127
Outputs:
- visibilities: float32 [512, 2, 256, 256], P(('chan', 'tm'))
The draws below stay inside these ranges and needn't reach their ends.
Inputs may be any that keep to these rules, and one draw needn't show every extreme that they name: `voltages`: samples that keep drops count as zero; a program may move only the kept samples, in any compact form. `flag_mask`: 1 keeps the block of 128 samples of an antenna, 0 drops it; some antennas are dropped in every block. The first flagged_prefix_counts samples of a kept block are flagged; flags and counts may be packed several to a word wherever they are moved.
All inputs are finite; a program needn't handle non-finite values.
Results may differ from the reference program's by a relative error of at most 0.0003.
Values may be sent and summed in bfloat16 or wider, within the bound.
A program may use at most 128 MiB of HBM per device.

```python
import jax
import jax.numpy as jnp
from jax import lax

ANTENNA_COUNT = 256
CHANNEL_COUNT = 512
FLAG_BLOCK_WIDTH = 128
FLAG_BLOCK_COUNT = 4
SAMPLE_COUNT = 512


def draw_voltages(key, part):
    value_key = jax.random.fold_in(key, 31)
    zero_key = jax.random.fold_in(key, 29)
    full_shape = (2, CHANNEL_COUNT, ANTENNA_COUNT, SAMPLE_COUNT)
    normal_values = jax.random.normal(value_key, full_shape, jnp.float32)
    values_drawn = jnp.clip(normal_values, -6.0, 6.0)
    silent = jax.random.randint(zero_key, (ANTENNA_COUNT, SAMPLE_COUNT), 0, 10) == 0
    return jnp.where(silent[None, None], 0.0, values_drawn).astype(jnp.bfloat16)


def draw_flag_mask(key, part):
    base = jax.random.fold_in(key, 17)
    initial_key, middle_key, final_key = jax.random.split(base, 3)
    valid_samples = (jax.random.randint(initial_key, (FLAG_BLOCK_COUNT, ANTENNA_COUNT), 0, 4) > 0).astype(jnp.int32)
    flagged_rows = jax.random.randint(middle_key, (ANTENNA_COUNT,), 0, 32) == 0
    selected_mask = jax.random.randint(final_key, (), 0, ANTENNA_COUNT)
    flagged_rows = flagged_rows | (jnp.arange(ANTENNA_COUNT) == selected_mask)
    return jnp.where(flagged_rows[None, :], 0, valid_samples).astype(jnp.int32)


def set_ends(result, rng, least, high):
    spot = [jax.random.randint(jax.random.fold_in(rng, axis), (), 0, length) for axis, length in enumerate(result.shape)]
    longest = result.shape.index(max(result.shape))
    neighbour = spot[:longest] + [(spot[longest] + 1) % result.shape[longest]] + spot[longest + 1:]
    return result.at[tuple(spot)].set(least).at[tuple(neighbour)].set(high)


def setup_inputs(seed: int = 0) -> dict:
    seeds = jax.random.split(jax.random.key(seed), 4)
    return {
        "voltages": draw_voltages(jax.random.fold_in(seeds[3], 71), 0),
        "flag_mask": draw_flag_mask(jax.random.fold_in(seeds[3], 71), 0),
        "flagged_prefix_counts": set_ends(jax.random.randint(seeds[2], (FLAG_BLOCK_COUNT, ANTENNA_COUNT), 0, FLAG_BLOCK_WIDTH), jax.random.fold_in(seeds[2], 1), 0, FLAG_BLOCK_WIDTH - 1).astype(jnp.int32),
    }


def pair_samples(flag_mask, flagged_prefix_counts):
    def add_block(total, block):
        live = block[0].astype(jnp.float32)
        cover = (FLAG_BLOCK_WIDTH - jnp.maximum(block[1][:, None], block[1][None, :])).astype(jnp.float32)
        return total + live[:, None] * live[None, :] * cover, 0

    start = jnp.zeros((flag_mask.shape[1], flag_mask.shape[1]), jnp.float32)
    total, unused = lax.scan(add_block, start, (flag_mask, flagged_prefix_counts))
    return total


def reference(voltages, flag_mask, flagged_prefix_counts):
    offsets = jnp.arange(FLAG_BLOCK_WIDTH, dtype=jnp.int32)
    retain_mask = (flag_mask.T[:, :, None] == 1) & (offsets[None, None, :] >= flagged_prefix_counts.T[:, :, None])
    retain_mask = retain_mask.reshape(ANTENNA_COUNT, SAMPLE_COUNT)
    width = 8

    def single_block(start):
        slab = lax.dynamic_slice_in_dim(voltages, start, width, 1)
        slab = jnp.where(retain_mask[None, None], slab, jnp.zeros((), slab.dtype)).astype(jnp.float32)
        real_part, imag_part = slab[0], slab[1]
        hp = lax.Precision.HIGHEST
        rr = jnp.einsum("cit,cjt->cij", real_part, real_part, precision=hp)
        ii = jnp.einsum("cit,cjt->cij", imag_part, imag_part, precision=hp)
        ir = jnp.einsum("cit,cjt->cij", imag_part, real_part, precision=hp)
        ri = jnp.einsum("cit,cjt->cij", real_part, imag_part, precision=hp)
        return jnp.stack([rr + ii, ir - ri], axis=1)

    block_offsets = jnp.arange(0, CHANNEL_COUNT, width, dtype=jnp.int32)
    visibility_matrix = lax.map(single_block, block_offsets).reshape(CHANNEL_COUNT, 2, ANTENNA_COUNT, ANTENNA_COUNT)
    pairs = pair_samples(flag_mask, flagged_prefix_counts)
    return visibility_matrix / jnp.maximum(pairs, 1.0)[None, None]
```

```python
import functools

import jax
import jax.numpy as jnp
from jax import lax
from jax.experimental import pallas as pl
from jax.experimental.pallas import tpu as pltpu
from jax.sharding import PartitionSpec as P

FLAG_BLOCK_WIDTH = 128
LANES = 128
SUBLANES = 8
MESH = pl.DeviceIdType.MESH
NT = (((1,), (1,)), ((), ()))


def exchange_kernel(
    n_chan, n_tm, groups, volt_ref, limit_ref, out_ref,
    held, table, cols, keep, inverse, send_sem, recv_sem, table_send, table_recv,
):
    n = n_chan * n_tm
    channels = held.shape[1]
    step = channels // groups
    antennas, samples = volt_ref.shape[2], volt_ref.shape[3]
    total_antennas = n_chan * antennas
    local_blocks = samples // FLAG_BLOCK_WIDTH
    my_chan, my_tm = lax.axis_index("chan"), lax.axis_index("tm")
    me = my_chan * n_tm + my_tm

    def swing(m):
        return (m + 1) // 2 * (1 - 2 * lax.rem(m + 1, 2))

    def hop(k):
        return n // 2 + swing(k - 1)

    def place(k):
        other = lax.rem(me + hop(k), n)
        return other, (other // n_tm, lax.rem(other, n_tm))

    barrier = pltpu.get_barrier_semaphore()

    def greet(k, carry):
        pl.semaphore_signal(barrier, inc=1, device_id=place(k)[1], device_id_type=MESH)
        return carry

    lax.fori_loop(1, n, greet, 0)
    pl.semaphore_wait(barrier, n - 1)

    def landing(g):
        return held.at[
            :, pl.ds(g * step, step), my_chan, :, pl.ds(pl.multiple_of(my_tm * samples, LANES), samples)
        ]

    def flag_copy(k):
        return pltpu.make_async_remote_copy(
            src_ref=limit_ref, dst_ref=table.at[me], send_sem=table_send.at[k], recv_sem=table_recv,
            device_id=place(k)[1], device_id_type=MESH,
        )

    def volt_copy(g, k):
        other, where = place(k)
        return pltpu.make_async_remote_copy(
            src_ref=volt_ref.at[:, pl.ds(other * channels + g * step, step)],
            dst_ref=landing(g), send_sem=send_sem.at[g, k], recv_sem=recv_sem.at[g],
            device_id=where, device_id_type=MESH,
        )

    def each(body):
        def run(k, carry):
            body(k)
            return carry

        lax.fori_loop(1, n, run, 0)

    each(lambda k: flag_copy(k).start())
    for g in range(groups):
        each(lambda k, g=g: volt_copy(g, k).start())
    pltpu.make_async_copy(limit_ref, table.at[me], table_recv).start()
    for g in range(groups):
        pltpu.make_async_copy(
            volt_ref.at[:, pl.ds(me * channels + g * step, step)], landing(g), recv_sem.at[g]
        ).start()

    pltpu.make_async_copy(table, table, table_recv).wait()
    rows = table[:, 0, :].astype(jnp.float32)
    padding = -n % LANES
    if padding:
        rows = jnp.concatenate([rows, jnp.zeros((padding, rows.shape[1]), jnp.float32)], axis=0)
    turned = rows.T
    lane = lax.broadcasted_iota(jnp.int32, (total_antennas, LANES), 1).astype(jnp.float32)
    pairs = jnp.zeros((total_antennas, total_antennas), jnp.float32)
    for t in range(n_tm):
        for b in range(local_blocks):
            q = t * local_blocks + b
            for c in range(n_chan):
                source = c * n_tm + t
                cols[c * antennas:(c + 1) * antennas, :] = jnp.broadcast_to(
                    turned[b * antennas:(b + 1) * antennas, source:source + 1], (antennas, LANES)
                )
            column = cols[...]
            keep[:, q * LANES:(q + 1) * LANES] = jnp.where(lane >= column, 1.0, 0.0).astype(keep.dtype)
            pairs += FLAG_BLOCK_WIDTH - jnp.maximum(column[:, :1], column.T[:1, :])
    inverse[...] = 1.0 / jnp.maximum(pairs, 1.0)

    def correlate(c, carry):
        size = (total_antennas, keep.shape[1])
        real = held[0, c].reshape(size) * keep[...]
        imag = held[1, c].reshape(size) * keep[...]
        same = lax.dot_general(real, real, NT, preferred_element_type=jnp.float32)
        same += lax.dot_general(imag, imag, NT, preferred_element_type=jnp.float32)
        cross = lax.dot_general(imag, real, NT, preferred_element_type=jnp.float32)
        out_ref[c, 0] = same * inverse[...]
        out_ref[c, 1] = (cross - cross.T) * inverse[...]
        return carry

    for g in range(groups):
        part = held.at[:, pl.ds(g * step, step)]
        pltpu.make_async_copy(part, part, recv_sem.at[g]).wait()
        lax.fori_loop(g * step, (g + 1) * step, correlate, 0)

    each(lambda k: flag_copy(k).wait_send())
    for g in range(groups):
        each(lambda k, g=g: volt_copy(g, k).wait_send())


def shards(n_chan, n_tm, voltages, flag_mask, flagged_prefix_counts):
    parts, all_channels, antennas, samples = voltages.shape
    n = n_chan * n_tm
    channels = all_channels // n
    total_antennas, total_samples = antennas * n_chan, samples * n_tm
    groups = max(g for g in (4, 2, 1) if channels % g == 0)
    limits = jnp.where(flag_mask == 1, flagged_prefix_counts, FLAG_BLOCK_WIDTH).reshape(1, -1)
    limits = jnp.pad(limits, ((0, 0), (0, -limits.shape[1] % LANES)))
    width = limits.shape[1]
    return pl.pallas_call(
        functools.partial(exchange_kernel, n_chan, n_tm, groups),
        out_shape=pltpu.VMEM((channels, 2, total_antennas, total_antennas), jnp.float32),
        in_specs=[pl.BlockSpec(memory_space=pl.ANY), pl.BlockSpec(memory_space=pltpu.VMEM)],
        out_specs=pl.BlockSpec(memory_space=pltpu.VMEM),
        scratch_shapes=[
            pltpu.VMEM((parts, channels, n_chan, antennas, total_samples), voltages.dtype),
            pltpu.VMEM((n, 1, width), jnp.int32),
            pltpu.VMEM((total_antennas, LANES), jnp.float32),
            pltpu.VMEM((total_antennas, total_samples), voltages.dtype),
            pltpu.VMEM((total_antennas, total_antennas), jnp.float32),
            pltpu.SemaphoreType.DMA((groups, n)),
            pltpu.SemaphoreType.DMA((groups,)),
            pltpu.SemaphoreType.DMA((n,)),
            pltpu.SemaphoreType.DMA,
        ],
        compiler_params=pltpu.CompilerParams(
            collective_id=0, has_side_effects=True, vmem_limit_bytes=48 * 1024 * 1024
        ),
    )(voltages, limits)


def rotate(x, shift):
    return pltpu.roll(x, shift, axis=1)


def pack_kernel(
    n_chan, n_tm, levels, volt_ref, mask_ref, count_ref, both_ref, table_ref, meta_ref, level_ref,
    held, theirs, mine, row, table, steps,
    load_sem, flag_send, flag_recv, pair_send, pair_recv, keep_sem, own_sem,
):
    n = n_chan * n_tm
    parts, all_channels, antennas, samples = volt_ref.shape
    channels = all_channels // n
    chips, groups, entries = mine.shape[0], mine.shape[1], mine.shape[2]
    width = SUBLANES // parts
    blocks = samples // FLAG_BLOCK_WIDTH
    segments = blocks * antennas
    my_chan, my_tm = lax.axis_index("chan"), lax.axis_index("tm")
    me = my_chan * n_tm + my_tm
    side = lax.rem(my_chan, 2)
    partner = (my_chan + 1 - 2 * side, my_tm)

    def place(k):
        other = lax.rem(me + k, n)
        return (other // n_tm, lax.rem(other, n_tm))

    barrier = pltpu.get_barrier_semaphore()

    def greet(k, carry):
        pl.semaphore_signal(barrier, inc=1, device_id=place(k), device_id_type=MESH)
        return carry

    lax.fori_loop(1, n, greet, 0)

    def load(d):
        part = pl.ds(d * channels, channels)
        return pltpu.make_async_copy(volt_ref.at[:, part], held.at[:, part], load_sem.at[d])

    def device_of(m, which):
        chan = m // n_tm * 2 + lax.rem(side + which, 2)
        return chan * n_tm + lax.rem(m, n_tm)

    def start_load(m, carry):
        load(device_of(m, 1)).start()
        load(device_of(m, 0)).start()
        return carry

    lax.fori_loop(0, chips, start_load, 0)

    lane = lax.broadcasted_iota(jnp.int32, (SUBLANES, LANES), 1)
    limits = jnp.full((SUBLANES, LANES), FLAG_BLOCK_WIDTH, jnp.int32)
    start = jnp.int32(0)
    for s in range(segments):
        b, i = s // antennas, s % antennas
        limit = jnp.where(mask_ref[b, i] == 1, count_ref[b, i], FLAG_BLOCK_WIDTH)
        limits = jnp.where(lane == s, limit, limits)
        first = start & (LANES - 1)
        spills = first + FLAG_BLOCK_WIDTH - limit > LANES
        steps[0, s] = (first - limit) & (LANES - 1)
        steps[1, s] = first
        steps[2, s] = jnp.where(spills, 0, first)
        start = start + FLAG_BLOCK_WIDTH - limit
    row[...] = limits[:1]

    old = lax.broadcasted_iota(jnp.int32, (SUBLANES * antennas, SUBLANES * antennas), 1)
    new = lax.broadcasted_iota(jnp.int32, (SUBLANES * antennas, SUBLANES * antennas), 0)
    turn = jnp.where(old == lax.rem(new, SUBLANES) * antennas + new // SUBLANES, 1.0, 0.0).astype(volt_ref.dtype)

    def pack(d, m, target):
        for g in range(groups):
            part = held[:, pl.ds(d * channels + g * width, width)].reshape(SUBLANES * antennas, samples)
            flat = jnp.dot(turn, part, preferred_element_type=jnp.float32)
            carry = jnp.zeros((SUBLANES, LANES), jnp.float32)
            for s in range(segments):
                b, i = s // antennas, s % antennas
                piece = flat[i * SUBLANES:(i + 1) * SUBLANES, b * LANES:(b + 1) * LANES]
                piece = rotate(piece, steps[0, s])
                target[m, g, s] = jnp.where(lane >= steps[1, s], piece, carry).astype(target.dtype)
                carry = jnp.where(lane >= steps[2, s], piece, carry)
            target[m, g, segments] = carry.astype(target.dtype)

    pl.semaphore_wait(barrier, n - 1)

    def flag_copy(k):
        return pltpu.make_async_remote_copy(
            src_ref=row, dst_ref=table.at[me], send_sem=flag_send.at[k], recv_sem=flag_recv,
            device_id=place(k), device_id_type=MESH,
        )

    def send_flags(k, carry):
        flag_copy(k).start()
        return carry

    lax.fori_loop(1, n, send_flags, 0)
    pltpu.make_async_copy(row, table.at[me], flag_recv).start()

    def pair_copy(m):
        return pltpu.make_async_remote_copy(
            src_ref=theirs.at[m], dst_ref=both_ref.at[1, m], send_sem=pair_send.at[m], recv_sem=pair_recv,
            device_id=partner, device_id_type=MESH,
        )

    def keep_copy(m):
        return pltpu.make_async_copy(mine.at[m], both_ref.at[0, m], keep_sem.at[m])

    def chip(m, carry):
        d = device_of(m, 1)
        load(d).wait()
        pack(d, m, theirs)
        pair_copy(m).start()
        d = device_of(m, 0)
        load(d).wait()
        pack(d, m, mine)
        keep_copy(m).start()
        return carry

    lax.fori_loop(0, chips, chip, 0)

    pltpu.make_async_copy(table, table, flag_recv).wait()
    rows = table[:, 0, :]
    lanes = lax.broadcasted_iota(jnp.int32, (n, LANES), 1)
    kept = (FLAG_BLOCK_WIDTH - rows).astype(jnp.float32).astype(jnp.bfloat16)
    above = jnp.where(
        lax.broadcasted_iota(jnp.int32, (LANES, LANES), 0) < lax.broadcasted_iota(jnp.int32, (LANES, LANES), 1), 1.0, 0.0
    ).astype(jnp.bfloat16)
    offset = jnp.dot(kept, above, preferred_element_type=jnp.float32).astype(jnp.int32)
    full = jnp.max((offset + (LANES - 1)) >> 7, axis=1, keepdims=True)
    full = jnp.broadcast_to(full, (n, LANES))
    to = lax.broadcasted_iota(jnp.int32, (n, n), 0)
    frm = lax.broadcasted_iota(jnp.int32, (n, n), 1)
    behind = jnp.where((frm == to - n_tm) & (lax.rem(to // n_tm, 2) == 1), 1.0, 0.0).astype(jnp.bfloat16)
    base = jnp.dot(behind, full.astype(jnp.float32).astype(jnp.bfloat16), preferred_element_type=jnp.float32).astype(jnp.int32)
    at = offset >> 7
    meta_ref[0] = ((base + at) << 16) | ((offset & (LANES - 1)) << 8) | rows
    place_of = jnp.full((n, LANES), -1, jnp.int32)
    for s in range(segments + 1):
        place_of += jnp.where(at[:, s:s + 1] <= lanes, 1, 0)
    meta_ref[1] = jnp.where(lanes == LANES - 1, full, place_of)
    table_ref[...] = rows
    need = jnp.max(base + full, axis=0, keepdims=True)
    level = jnp.zeros((1, LANES), jnp.int32)
    for q in levels[:-1]:
        level += jnp.where(need > q, 1, 0)
    level_ref[...] = level

    def drain(m, carry):
        pair_copy(m).wait_send()
        keep_copy(m).wait()
        return carry

    lax.fori_loop(0, chips, drain, 0)
    pltpu.make_async_copy(both_ref.at[1], both_ref.at[1], pair_recv).wait()

    def drain_flags(k, carry):
        flag_copy(k).wait_send()
        return carry

    lax.fori_loop(1, n, drain_flags, 0)


def unite_kernel(n_chan, n_tm, antennas, samples, sent, both_ref, table_ref, meta_ref, out_ref, *scratch):
    groups = both_ref.shape[2]
    landing = scratch[:groups]
    both, ready, square, cols, inverse, both_sem, send_sem, recv_sem = scratch[groups:]
    n, chips = n_chan * n_tm, both_ref.shape[1]
    total_antennas, total_samples = square.shape[1], square.shape[2]
    blocks = samples // FLAG_BLOCK_WIDTH
    width = out_ref.shape[0] // groups
    my_chan, my_tm = lax.axis_index("chan"), lax.axis_index("tm")
    side = lax.rem(my_chan, 2)
    here = my_chan // 2 * n_tm + my_tm

    def swing(m):
        return (m + 1) // 2 * (1 - 2 * lax.rem(m + 1, 2))

    def place(k):
        other = lax.rem(here + chips // 2 + swing(k - 1), chips)
        return other, (other // n_tm * 2 + side, lax.rem(other, n_tm))

    barrier = pltpu.get_barrier_semaphore()

    def greet(k, carry):
        pl.semaphore_signal(barrier, inc=1, device_id=place(k)[1], device_id_type=MESH)
        return carry

    lax.fori_loop(1, chips, greet, 0)
    fetch = pltpu.make_async_copy(both_ref, both, both_sem)
    fetch.start()
    first_device = (my_chan - side) * n_tm + my_tm
    split = meta_ref[1, first_device, LANES - 1]
    fetch.wait()

    def gather(g):
        def pick(r, carry):
            second = jnp.where(r < split, 0, 1)
            entry = meta_ref[1, first_device + second * n_tm, r - second * split]
            ready[g, :, r] = both[jnp.where(second == side, 0, 1), :, g, entry]
            return carry

        lax.fori_loop(0, sent, pick, 0)

    def copy(g, k):
        other, where = place(k)
        return pltpu.make_async_remote_copy(
            src_ref=ready.at[g, other], dst_ref=landing[g].at[here, pl.ds(0, sent)],
            send_sem=send_sem.at[g, k], recv_sem=recv_sem.at[g], device_id=where, device_id_type=MESH,
        )

    def each(body):
        def run(k, carry):
            body(k)
            return carry

        lax.fori_loop(1, chips, run, 0)

    for g in range(groups):
        gather(g)
        if g == 0:
            pl.semaphore_wait(barrier, chips - 1)
        each(lambda k, g=g: copy(g, k).start())
        pltpu.make_async_copy(ready.at[g, here], landing[g].at[here, pl.ds(0, sent)], recv_sem.at[g]).start()

    rows = table_ref[...].astype(jnp.float32)
    padding = -n % LANES
    if padding:
        rows = jnp.concatenate([rows, jnp.zeros((padding, rows.shape[1]), jnp.float32)], axis=0)
    turned = rows.T
    pairs = jnp.zeros((total_antennas, total_antennas), jnp.float32)
    for t in range(n_tm):
        for b in range(blocks):
            for c in range(n_chan):
                source = c * n_tm + t
                cols[c * antennas:(c + 1) * antennas, :] = jnp.broadcast_to(
                    turned[b * antennas:(b + 1) * antennas, source:source + 1], (antennas, LANES)
                )
            column = cols[...]
            pairs += FLAG_BLOCK_WIDTH - jnp.maximum(column[:, :1], column.T[:1, :])
    inverse[...] = 1.0 / jnp.maximum(pairs, 1.0)

    lane = lax.broadcasted_iota(jnp.int32, (SUBLANES, LANES), 1)
    old = lax.broadcasted_iota(jnp.int32, (SUBLANES * antennas, SUBLANES * antennas), 1)
    new = lax.broadcasted_iota(jnp.int32, (SUBLANES * antennas, SUBLANES * antennas), 0)
    turn = jnp.where(new == lax.rem(old, SUBLANES) * antennas + old // SUBLANES, 1.0, 0.0).astype(square.dtype)

    for g in range(groups):
        part = landing[g].at[:, pl.ds(0, sent)]
        pltpu.make_async_copy(part, part, recv_sem.at[g]).wait()

        def expand(d, carry, g=g):
            chan, t = d // n_tm, lax.rem(d, n_tm)
            m = chan // 2 * n_tm + t
            bands = []
            for i in range(antennas):
                band = []
                for b in range(blocks):
                    word = meta_ref[0, d, b * antennas + i]
                    at, first, limit = word >> 16, (word >> 8) & 255, word & 255
                    low = landing[g][m, at].astype(jnp.float32)
                    high = landing[g][m, at + 1].astype(jnp.float32)
                    piece = rotate(jnp.where(lane >= first, low, high), (limit - first) & (LANES - 1))
                    band.append(jnp.where(lane >= limit, piece, 0.0))
                bands.append(jnp.concatenate(band, axis=1))
            flat = jnp.concatenate(bands, axis=0).astype(square.dtype)
            flat = jnp.dot(turn, flat, preferred_element_type=jnp.float32).astype(square.dtype)
            for q in range(SUBLANES):
                square[
                    q, pl.ds(pl.multiple_of(chan * antennas, antennas), antennas),
                    pl.ds(pl.multiple_of(t * samples, LANES), samples),
                ] = flat[q * antennas:(q + 1) * antennas]
            return carry

        lax.fori_loop(0, n, expand, 0)

        def correlate(c, carry, g=g):
            real, imag = square[c], square[width + c]
            same = lax.dot_general(real, real, NT, preferred_element_type=jnp.float32)
            same += lax.dot_general(imag, imag, NT, preferred_element_type=jnp.float32)
            cross = lax.dot_general(imag, real, NT, preferred_element_type=jnp.float32)
            out_ref[g * width + c, 0] = same * inverse[...]
            out_ref[g * width + c, 1] = (cross - cross.T) * inverse[...]
            return carry

        lax.fori_loop(0, width, correlate, 0)

    for g in range(groups):
        each(lambda k, g=g: copy(g, k).wait_send())


def packed_shards(n_chan, n_tm, voltages, flag_mask, flagged_prefix_counts):
    parts, all_channels, antennas, samples = voltages.shape
    n = n_chan * n_tm
    chips = n // 2
    channels = all_channels // n
    width = SUBLANES // parts
    groups = channels // width
    blocks = samples // FLAG_BLOCK_WIDTH
    segments = blocks * antennas
    most = 2 * segments
    levels = [most]
    while levels[-1] > 8:
        levels.append(max(8, min(levels[-1] - 1, levels[-1] * 15 // 16)))
    levels = tuple(sorted(levels))
    dtype = voltages.dtype
    entries = segments + 1
    smem = pl.BlockSpec(memory_space=pltpu.SMEM)
    vmem = pl.BlockSpec(memory_space=pltpu.VMEM)
    hbm = pl.BlockSpec(memory_space=pl.ANY)
    both, table, meta, level = pl.pallas_call(
        functools.partial(pack_kernel, n_chan, n_tm, levels),
        out_shape=(
            jax.ShapeDtypeStruct((2, chips, groups, entries, SUBLANES, LANES), dtype),
            jax.ShapeDtypeStruct((n, LANES), jnp.int32),
            jax.ShapeDtypeStruct((2, n, LANES), jnp.int32),
            jax.ShapeDtypeStruct((1, LANES), jnp.int32),
        ),
        in_specs=[hbm, smem, smem],
        out_specs=(hbm, vmem, vmem, vmem),
        scratch_shapes=[
            pltpu.VMEM(voltages.shape, dtype),
            pltpu.VMEM((chips, groups, entries, SUBLANES, LANES), dtype),
            pltpu.VMEM((chips, groups, entries, SUBLANES, LANES), dtype),
            pltpu.VMEM((1, LANES), jnp.int32),
            pltpu.VMEM((n, 1, LANES), jnp.int32),
            pltpu.SMEM((3, segments), jnp.int32),
            pltpu.SemaphoreType.DMA((n,)),
            pltpu.SemaphoreType.DMA((n,)),
            pltpu.SemaphoreType.DMA,
            pltpu.SemaphoreType.DMA((chips,)),
            pltpu.SemaphoreType.DMA,
            pltpu.SemaphoreType.DMA((chips,)),
            pltpu.SemaphoreType.DMA,
        ],
        compiler_params=pltpu.CompilerParams(
            collective_id=0, has_side_effects=True, vmem_limit_bytes=40 * 1024 * 1024
        ),
    )(voltages, flag_mask, flagged_prefix_counts)
    total_antennas, total_samples = antennas * n_chan, samples * n_tm

    def unite(index, sent):
        return pl.pallas_call(
            functools.partial(unite_kernel, n_chan, n_tm, antennas, samples, sent),
            out_shape=pltpu.VMEM((channels, 2, total_antennas, total_antennas), jnp.float32),
            in_specs=[hbm, vmem, smem],
            out_specs=vmem,
            scratch_shapes=[pltpu.VMEM((chips, sent + 2, SUBLANES, LANES), dtype)] * groups + [
                pltpu.VMEM((2, chips, groups, entries, SUBLANES, LANES), dtype),
                pltpu.VMEM((groups, chips, sent, SUBLANES, LANES), dtype),
                pltpu.VMEM((SUBLANES, total_antennas, total_samples), dtype),
                pltpu.VMEM((total_antennas, LANES), jnp.float32),
                pltpu.VMEM((total_antennas, total_antennas), jnp.float32),
                pltpu.SemaphoreType.DMA,
                pltpu.SemaphoreType.DMA((groups, chips)),
                pltpu.SemaphoreType.DMA((groups,)),
            ],
            compiler_params=pltpu.CompilerParams(
                collective_id=1 + index, has_side_effects=True, vmem_limit_bytes=48 * 1024 * 1024
            ),
        )

    branches = [unite(index, sent) for index, sent in enumerate(levels)]
    return lax.switch(level[0, 0], branches, both, table, meta)


def packable(n_chan, n_tm, parts, all_channels, antennas, samples):
    n = n_chan * n_tm
    if n_chan % 2 or all_channels % n or SUBLANES % parts:
        return False
    segments = samples // FLAG_BLOCK_WIDTH * antennas
    return all_channels // n % (SUBLANES // parts) == 0 and antennas % 16 == 0 and segments < LANES - 1


def body(n_chan, n_tm, voltages, flag_mask, flagged_prefix_counts):
    chosen = packed_shards if packable(n_chan, n_tm, *voltages.shape) else shards
    return chosen(n_chan, n_tm, voltages, flag_mask, flagged_prefix_counts)


def solution(mesh):
    placed = (P(None, None, "chan", "tm"), P("tm", "chan"), P("tm", "chan"))
    return jax.shard_map(
        functools.partial(body, mesh.shape["chan"], mesh.shape["tm"]),
        mesh=mesh,
        in_specs=placed,
        out_specs=P(("chan", "tm"), None, None, None),
        check_vma=False,
    )
```

```python
import functools

import jax
import jax.numpy as jnp
from jax import lax
from jax.experimental import pallas as pl
from jax.experimental.pallas import tpu as pltpu
from jax.sharding import PartitionSpec as P

FLAG_BLOCK_WIDTH = 128
LANES = 128
SUBLANES = 8
AT, FIRST, LIMIT = 22, 15, 7
BATCHES = 4
LEVEL_STEPS = (8, 16, 22, 24, 25, 26, 27, 28, 29, 30, 31, 32, 34, 37, 42, 50, 64)
MESH = pl.DeviceIdType.MESH
NT = (((1,), (1,)), ((), ()))


def exchange_kernel(
    n_chan, n_tm, groups, volt_ref, limit_ref, out_ref,
    held, table, cols, keep, inverse, send_sem, recv_sem, table_send, table_recv,
):
    n = n_chan * n_tm
    channels = held.shape[1]
    step = channels // groups
    antennas, samples = volt_ref.shape[2], volt_ref.shape[3]
    total_antennas = n_chan * antennas
    local_blocks = samples // FLAG_BLOCK_WIDTH
    my_chan, my_tm = lax.axis_index("chan"), lax.axis_index("tm")
    me = my_chan * n_tm + my_tm

    def swing(m):
        return (m + 1) // 2 * (1 - 2 * lax.rem(m + 1, 2))

    def hop(k):
        return n // 2 + swing(k - 1)

    def place(k):
        other = lax.rem(me + hop(k), n)
        return other, (other // n_tm, lax.rem(other, n_tm))

    barrier = pltpu.get_barrier_semaphore()

    def greet(k, carry):
        pl.semaphore_signal(barrier, inc=1, device_id=place(k)[1], device_id_type=MESH)
        return carry

    lax.fori_loop(1, n, greet, 0)
    pl.semaphore_wait(barrier, n - 1)

    def landing(g):
        return held.at[
            :, pl.ds(g * step, step), my_chan, :, pl.ds(pl.multiple_of(my_tm * samples, LANES), samples)
        ]

    def flag_copy(k):
        return pltpu.make_async_remote_copy(
            src_ref=limit_ref, dst_ref=table.at[me], send_sem=table_send.at[k], recv_sem=table_recv,
            device_id=place(k)[1], device_id_type=MESH,
        )

    def volt_copy(g, k):
        other, where = place(k)
        return pltpu.make_async_remote_copy(
            src_ref=volt_ref.at[:, pl.ds(other * channels + g * step, step)],
            dst_ref=landing(g), send_sem=send_sem.at[g, k], recv_sem=recv_sem.at[g],
            device_id=where, device_id_type=MESH,
        )

    def each(body):
        def run(k, carry):
            body(k)
            return carry

        lax.fori_loop(1, n, run, 0)

    each(lambda k: flag_copy(k).start())
    for g in range(groups):
        each(lambda k, g=g: volt_copy(g, k).start())
    pltpu.make_async_copy(limit_ref, table.at[me], table_recv).start()
    for g in range(groups):
        pltpu.make_async_copy(
            volt_ref.at[:, pl.ds(me * channels + g * step, step)], landing(g), recv_sem.at[g]
        ).start()

    pltpu.make_async_copy(table, table, table_recv).wait()
    rows = table[:, 0, :].astype(jnp.float32)
    padding = -n % LANES
    if padding:
        rows = jnp.concatenate([rows, jnp.zeros((padding, rows.shape[1]), jnp.float32)], axis=0)
    turned = rows.T
    lane = lax.broadcasted_iota(jnp.int32, (total_antennas, LANES), 1).astype(jnp.float32)
    pairs = jnp.zeros((total_antennas, total_antennas), jnp.float32)
    for t in range(n_tm):
        for b in range(local_blocks):
            q = t * local_blocks + b
            for c in range(n_chan):
                source = c * n_tm + t
                cols[c * antennas:(c + 1) * antennas, :] = jnp.broadcast_to(
                    turned[b * antennas:(b + 1) * antennas, source:source + 1], (antennas, LANES)
                )
            column = cols[...]
            keep[:, q * LANES:(q + 1) * LANES] = jnp.where(lane >= column, 1.0, 0.0).astype(keep.dtype)
            pairs += FLAG_BLOCK_WIDTH - jnp.maximum(column[:, :1], column.T[:1, :])
    inverse[...] = 1.0 / jnp.maximum(pairs, 1.0)

    def correlate(c, carry):
        size = (total_antennas, keep.shape[1])
        real = held[0, c].reshape(size) * keep[...]
        imag = held[1, c].reshape(size) * keep[...]
        same = lax.dot_general(real, real, NT, preferred_element_type=jnp.float32)
        same += lax.dot_general(imag, imag, NT, preferred_element_type=jnp.float32)
        cross = lax.dot_general(imag, real, NT, preferred_element_type=jnp.float32)
        out_ref[c, 0] = same * inverse[...]
        out_ref[c, 1] = (cross - cross.T) * inverse[...]
        return carry

    for g in range(groups):
        part = held.at[:, pl.ds(g * step, step)]
        pltpu.make_async_copy(part, part, recv_sem.at[g]).wait()
        lax.fori_loop(g * step, (g + 1) * step, correlate, 0)

    each(lambda k: flag_copy(k).wait_send())
    for g in range(groups):
        each(lambda k, g=g: volt_copy(g, k).wait_send())


def shards(n_chan, n_tm, voltages, flag_mask, flagged_prefix_counts):
    parts, all_channels, antennas, samples = voltages.shape
    n = n_chan * n_tm
    channels = all_channels // n
    total_antennas, total_samples = antennas * n_chan, samples * n_tm
    groups = max(g for g in (4, 2, 1) if channels % g == 0)
    limits = jnp.where(flag_mask == 1, flagged_prefix_counts, FLAG_BLOCK_WIDTH).reshape(1, -1)
    limits = jnp.pad(limits, ((0, 0), (0, -limits.shape[1] % LANES)))
    width = limits.shape[1]
    return pl.pallas_call(
        functools.partial(exchange_kernel, n_chan, n_tm, groups),
        out_shape=pltpu.VMEM((channels, 2, total_antennas, total_antennas), jnp.float32),
        in_specs=[pl.BlockSpec(memory_space=pl.ANY), pl.BlockSpec(memory_space=pltpu.VMEM)],
        out_specs=pl.BlockSpec(memory_space=pltpu.VMEM),
        scratch_shapes=[
            pltpu.VMEM((parts, channels, n_chan, antennas, total_samples), voltages.dtype),
            pltpu.VMEM((n, 1, width), jnp.int32),
            pltpu.VMEM((total_antennas, LANES), jnp.float32),
            pltpu.VMEM((total_antennas, total_samples), voltages.dtype),
            pltpu.VMEM((total_antennas, total_antennas), jnp.float32),
            pltpu.SemaphoreType.DMA((groups, n)),
            pltpu.SemaphoreType.DMA((groups,)),
            pltpu.SemaphoreType.DMA((n,)),
            pltpu.SemaphoreType.DMA,
        ],
        compiler_params=pltpu.CompilerParams(
            collective_id=0, has_side_effects=True, vmem_limit_bytes=48 * 1024 * 1024
        ),
    )(voltages, limits)


def pack_kernel(
    n_chan, n_tm, levels, volt_ref, mask_ref, count_ref, first_ref, rest_ref, theirs_ref, table_ref, meta_ref, level_ref,
    held, theirs, mine, even, odd, row, table, flags, steps,
    load_sem, word_sem, flag_send, flag_recv, pair_send, pair_recv, keep_sem,
):
    n = n_chan * n_tm
    parts, all_channels, antennas, samples = volt_ref.shape
    channels = all_channels // n
    chips, groups = mine.shape[0], mine.shape[1]
    width = SUBLANES // parts
    blocks = samples // FLAG_BLOCK_WIDTH
    segments = blocks * antennas
    my_chan, my_tm = lax.axis_index("chan"), lax.axis_index("tm")
    me = my_chan * n_tm + my_tm
    side = lax.rem(my_chan, 2)
    partner = (my_chan + 1 - 2 * side, my_tm)

    def loop(low, high, do):
        def run(k, carry):
            do(k)
            return carry

        lax.fori_loop(low, high, run, 0)

    def others(do):
        def at(j, low):
            chan = my_chan + j
            chan = jnp.where(chan >= n_chan, chan - n_chan, chan)
            for u in range(low, n_tm):
                t = my_tm + u
                do(j * n_tm + u, (chan, jnp.where(t >= n_tm, t - n_tm, t)))

        loop(1, n_chan, lambda j: at(j, 0))
        at(0, 1)

    barrier = pltpu.get_barrier_semaphore()
    others(lambda k, where: pl.semaphore_signal(barrier, inc=1, device_id=where, device_id_type=MESH))
    words = [pltpu.make_async_copy(ref, flags.at[q], word_sem.at[q]) for q, ref in enumerate((mask_ref, count_ref))]
    for word in words:
        word.start()

    def load(d):
        part = pl.ds(d * channels, channels)
        return pltpu.make_async_copy(volt_ref.at[:, part], held.at[:, part], load_sem.at[d])

    def device_of(j):
        m = lax.rem(j, chips)
        chan = m // n_tm * 2 + lax.rem(side + 1 + j // chips, 2)
        return chan * n_tm + lax.rem(m, n_tm)

    loop(0, n, lambda j: load(device_of(j)).start())
    for word in words:
        word.wait()

    lane = lax.broadcasted_iota(jnp.int32, (SUBLANES, LANES), 1)
    limits = jnp.full((SUBLANES, LANES), FLAG_BLOCK_WIDTH, jnp.int32)
    start = jnp.int32(0)
    for s in range(segments):
        b, i = s // antennas, s % antennas
        limit = jnp.where(flags[0, b, i] == 1, flags[1, b, i], FLAG_BLOCK_WIDTH)
        limits = jnp.where(lane == s, limit, limits)
        first = start & (LANES - 1)
        spills = first + FLAG_BLOCK_WIDTH - limit > LANES
        steps[0, s] = (first - limit) & (LANES - 1)
        steps[1, s] = first
        steps[2, s] = jnp.where(spills, 0, first)
        start = start + FLAG_BLOCK_WIDTH - limit
    row[...] = limits[:1]

    old = lax.broadcasted_iota(jnp.int32, (SUBLANES * antennas, SUBLANES * antennas), 1)
    new = lax.broadcasted_iota(jnp.int32, (SUBLANES * antennas, SUBLANES * antennas), 0)
    turn = jnp.where(old == lax.rem(new, SUBLANES) * antennas + new // SUBLANES, 1.0, 0.0).astype(volt_ref.dtype)

    def flatten(j, flat):
        d = device_of(j)
        load(d).wait()
        for g in range(groups):
            part = held[:, pl.ds(d * channels + g * width, width)].reshape(SUBLANES * antennas, samples)
            flat[g] = jnp.dot(turn, part, preferred_element_type=jnp.float32)

    def merge(flat, target, m):
        carry = [jnp.zeros((SUBLANES, LANES), jnp.float32)] * groups
        for s in range(segments):
            b, i = s // antennas, s % antennas
            shift, opens, stays = steps[0, s], lane >= steps[1, s], lane >= steps[2, s]
            for g in range(groups):
                piece = flat[g, i * SUBLANES:(i + 1) * SUBLANES, b * LANES:(b + 1) * LANES]
                piece = pltpu.roll(piece, shift, axis=1)
                target[m, g, s] = jnp.where(opens, piece, carry[g]).astype(target.dtype)
                carry[g] = jnp.where(stays, piece, carry[g])
        for g in range(groups):
            target[m, g, segments] = carry[g].astype(target.dtype)

    def flag_copy(k, where):
        return pltpu.make_async_remote_copy(
            src_ref=row, dst_ref=table.at[me], send_sem=flag_send.at[k], recv_sem=flag_recv,
            device_id=where, device_id_type=MESH,
        )

    pair_copy = pltpu.make_async_remote_copy(
        src_ref=theirs.at[:, 0], dst_ref=first_ref.at[1], send_sem=pair_send, recv_sem=pair_recv,
        device_id=partner, device_id_type=MESH,
    )
    keeps = [
        pltpu.make_async_copy(ref, where, keep_sem.at[q])
        for q, (ref, where) in enumerate((
            (theirs.at[:, pl.ds(1, groups - 1)], theirs_ref),
            (mine.at[:, 0], first_ref.at[0]),
            (mine.at[:, pl.ds(1, groups - 1)], rest_ref),
        ))
    ]

    def pack_theirs(h):
        flatten(2 * h + 1, odd)
        merge(even, theirs, 2 * h)
        flatten(2 * h + 2, even)
        merge(odd, theirs, 2 * h + 1)

    def pack_mine(h):
        flatten(chips + 2 * h + 1, odd)
        merge(even, mine, 2 * h)
        flatten(chips + 2 * h + 2, even)
        merge(odd, mine, 2 * h + 1)

    flatten(0, even)
    loop(0, chips // 2, pack_theirs)
    pl.semaphore_wait(barrier, n - 1)
    others(lambda k, where: flag_copy(k, where).start())
    pair_copy.start()
    pltpu.make_async_copy(row, table.at[me], flag_recv).start()
    keeps[0].start()
    loop(0, chips // 2 - 1, pack_mine)
    flatten(n - 1, odd)
    merge(even, mine, chips - 2)
    merge(odd, mine, chips - 1)
    keeps[1].start()
    keeps[2].start()

    pltpu.make_async_copy(table, table, flag_recv).wait()
    rows = table[:, 0, :]
    lanes = lax.broadcasted_iota(jnp.int32, (n, LANES), 1)
    kept = (FLAG_BLOCK_WIDTH - rows).astype(jnp.float32).astype(jnp.bfloat16)
    above = jnp.where(
        lax.broadcasted_iota(jnp.int32, (LANES, LANES), 0) < lax.broadcasted_iota(jnp.int32, (LANES, LANES), 1), 1.0, 0.0
    ).astype(jnp.bfloat16)
    offset = jnp.dot(kept, above, preferred_element_type=jnp.float32).astype(jnp.int32)
    full = jnp.max((offset + (LANES - 1)) >> 7, axis=1, keepdims=True)
    full = jnp.broadcast_to(full, (n, LANES))
    to = lax.broadcasted_iota(jnp.int32, (n, n), 0)
    frm = lax.broadcasted_iota(jnp.int32, (n, n), 1)
    behind = jnp.where((frm == to - n_tm) & (lax.rem(to // n_tm, 2) == 1), 1.0, 0.0).astype(jnp.bfloat16)
    base = jnp.dot(behind, full.astype(jnp.float32).astype(jnp.bfloat16), preferred_element_type=jnp.float32).astype(jnp.int32)
    at = offset >> 7
    first = offset & (LANES - 1)
    meta_ref[0] = ((base + at) << AT) | (first << FIRST) | (rows << LIMIT) | ((rows - first) & (LANES - 1))
    place_of = jnp.full((n, LANES), -1, jnp.int32)
    for s in range(segments + 1):
        place_of += jnp.where(at[:, s:s + 1] <= lanes, 1, 0)
    meta_ref[1] = jnp.where(lanes == LANES - 1, full, place_of)
    table_ref[...] = rows
    need = jnp.max(base + full, axis=0, keepdims=True)
    level = jnp.zeros((1, LANES), jnp.int32)
    for q in levels[:-1]:
        level += jnp.where(need > q, 1, 0)
    level_ref[...] = level

    for keep in keeps:
        keep.wait()
    pair_copy.wait()
    others(lambda k, where: flag_copy(k, where).wait_send())


def unite_kernel(
    n_chan, n_tm, antennas, samples, sent, first_ref, rest_ref, theirs_ref, table_ref, meta_ref, out_ref,
    first, rest, ready, landing, work, even, odd, square, cols, inverse, result,
    fetch_sem, pair_send, pair_recv, send_sem, recv_sem, out_sem,
):
    groups = landing.shape[0]
    n, chips = n_chan * n_tm, first_ref.shape[1]
    half, batch = chips // 2, chips // recv_sem.shape[1]
    total_antennas, total_samples = square.shape[1], square.shape[2]
    blocks = samples // FLAG_BLOCK_WIDTH
    channels = out_ref.shape[0]
    width = channels // groups
    my_chan, my_tm = lax.axis_index("chan"), lax.axis_index("tm")
    side = lax.rem(my_chan, 2)
    here = my_chan // 2 * n_tm + my_tm
    my_half, my_place = here // half, lax.rem(here, half)
    partner = (my_chan + 1 - 2 * side, my_tm)

    def loop(low, high, do):
        def run(k, carry):
            do(k)
            return carry

        lax.fori_loop(low, high, run, 0)

    def chip_at(slot, step):
        other_half = lax.rem(my_half + slot // half, 2)
        return other_half * half + lax.rem(my_place + half + step * lax.rem(slot, half), half)

    def device_at(chip):
        return (chip // n_tm * 2 + side, lax.rem(chip, n_tm))

    barrier = pltpu.get_barrier_semaphore()
    loop(1, chips, lambda slot: pl.semaphore_signal(
        barrier, inc=1, device_id=device_at(chip_at(slot, 1)), device_id_type=MESH
    ))
    pl.semaphore_signal(barrier, inc=1, device_id=partner, device_id_type=MESH)
    fetches = [
        pltpu.make_async_copy(first_ref, first, fetch_sem.at[0]),
        pltpu.make_async_copy(rest_ref, rest.at[0], fetch_sem.at[1]),
    ]
    for fetch in fetches:
        fetch.start()
    pair_copy = pltpu.make_async_remote_copy(
        src_ref=theirs_ref, dst_ref=rest.at[1], send_sem=pair_send, recv_sem=pair_recv,
        device_id=partner, device_id_type=MESH,
    )
    low_device = (my_chan - side) * n_tm + my_tm
    split = meta_ref[1, low_device, LANES - 1]

    def gather(g, source):
        def pick(r):
            second = jnp.where(r < split, 0, 1)
            entry = meta_ref[1, low_device + second * n_tm, r - second * split]
            ready[g, :, r] = source(jnp.where(second == side, 0, 1), entry)

        loop(0, sent, pick)

    def copy(g, slot):
        chip = chip_at(slot, 1)
        return pltpu.make_async_remote_copy(
            src_ref=ready.at[g, chip], dst_ref=landing.at[g, slot, pl.ds(0, sent)],
            send_sem=send_sem.at[g, slot], recv_sem=recv_sem.at[g, slot // batch],
            device_id=device_at(chip), device_id_type=MESH,
        )

    def launch(g):
        loop(half, chips, lambda slot: copy(g, slot).start())
        loop(1, half, lambda slot: copy(g, slot).start())
        pltpu.make_async_copy(ready.at[g, here], landing.at[g, 0, pl.ds(0, sent)], recv_sem.at[g, 0]).start()

    def gather_and_launch(g):
        gather(g, lambda w, entry: rest[w, :, g - 1, entry])
        launch(g)

    fetches[0].wait()
    gather(0, lambda w, entry: first[w, :, entry])
    pl.semaphore_wait(barrier, chips)
    pair_copy.start()
    launch(0)
    fetches[1].wait()
    pair_copy.wait_recv()
    loop(1, groups, gather_and_launch)

    rows = table_ref[...].astype(jnp.float32)
    padding = -n % LANES
    if padding:
        rows = jnp.concatenate([rows, jnp.zeros((padding, rows.shape[1]), jnp.float32)], axis=0)
    turned = rows.T
    pairs = jnp.zeros((total_antennas, total_antennas), jnp.float32)
    for t in range(n_tm):
        for b in range(blocks):
            for c in range(n_chan):
                source = c * n_tm + t
                cols[c * antennas:(c + 1) * antennas, :] = jnp.broadcast_to(
                    turned[b * antennas:(b + 1) * antennas, source:source + 1], (antennas, LANES)
                )
            column = cols[...]
            pairs += FLAG_BLOCK_WIDTH - jnp.maximum(column[:, :1], column.T[:1, :])
    inverse[...] = 1.0 / jnp.maximum(pairs, 1.0)

    lane = lax.broadcasted_iota(jnp.int32, (SUBLANES, LANES), 1)
    old = lax.broadcasted_iota(jnp.int32, (SUBLANES * antennas, SUBLANES * antennas), 1)
    new = lax.broadcasted_iota(jnp.int32, (SUBLANES * antennas, SUBLANES * antennas), 0)
    turn = jnp.where(new == lax.rem(old, SUBLANES) * antennas + old // SUBLANES, 1.0, 0.0).astype(square.dtype)

    lane_first = (lane << FIRST) | ((1 << FIRST) - 1)
    lane_limit = (lane << LIMIT) | ((1 << LIMIT) - 1)
    first_bits, limit_bits = (1 << AT) - (1 << FIRST), (1 << FIRST) - (1 << LIMIT)

    def source(part, q):
        chip = chip_at(part * batch + q // 2, -1)
        return chip // n_tm * 2 + lax.rem(q, 2), lax.rem(chip, n_tm)

    def expand(part, q, z):
        q = jnp.minimum(q, 2 * batch - 1)
        chan, t = source(part, q)
        d = chan * n_tm + t
        origin = q // 2 * (sent + 2)
        for i in range(antennas):
            for b in range(blocks):
                word = meta_ref[0, d, b * antennas + i]
                at = origin + (word >> AT)
                spread = jnp.full(lane.shape, word, jnp.int32)
                piece = jnp.where((spread & first_bits) <= lane_first, work[at], work[at + 1])
                piece = pltpu.roll(piece, word, axis=1)
                piece = jnp.where((spread & limit_bits) <= lane_limit, piece, 0.0)
                z[i * SUBLANES:(i + 1) * SUBLANES, b * LANES:(b + 1) * LANES] = piece.astype(z.dtype)

    def settle(part, q, z):
        chan, t = source(part, q)
        flat = jnp.dot(turn, z[...], preferred_element_type=jnp.float32).astype(square.dtype)
        for p in range(SUBLANES):
            square[
                p, pl.ds(pl.multiple_of(chan * antennas, antennas), antennas),
                pl.ds(pl.multiple_of(t * samples, LANES), samples),
            ] = flat[p * antennas:(p + 1) * antennas]

    def receive(g, part):
        arrived = landing.at[g, pl.ds(part * batch, batch), pl.ds(0, sent)]
        pltpu.make_async_copy(arrived, arrived, recv_sem.at[g, part]).wait()
        for j in range(batch):
            work[j * (sent + 2):j * (sent + 2) + sent] = landing[g, part * batch + j, :sent].astype(jnp.float32)
        expand(part, 0, even)

        def two(h):
            expand(part, 2 * h + 1, odd)
            settle(part, 2 * h, even)
            expand(part, 2 * h + 2, even)
            settle(part, 2 * h + 1, odd)

        loop(0, batch, two)

    def put(channel):
        return pltpu.make_async_copy(result.at[channel], out_ref.at[channel], out_sem.at[channel])

    def finish(g):
        loop(0, chips // batch, lambda part: receive(g, part))

        def correlate(c):
            real, imag = square[c], square[width + c]
            same = lax.dot_general(real, real, NT, preferred_element_type=jnp.float32)
            same += lax.dot_general(imag, imag, NT, preferred_element_type=jnp.float32)
            cross = lax.dot_general(imag, real, NT, preferred_element_type=jnp.float32)
            channel = g * width + c
            result[channel, 0] = same * inverse[...]
            result[channel, 1] = (cross - cross.T) * inverse[...]
            put(channel).start()

        loop(0, width, correlate)

    loop(0, groups, finish)
    pair_copy.wait_send()
    loop(0, groups, lambda g: loop(1, chips, lambda slot: copy(g, slot).wait_send()))
    loop(0, channels, lambda channel: put(channel).wait())


def packed_shards(n_chan, n_tm, voltages, flag_mask, flagged_prefix_counts):
    parts, all_channels, antennas, samples = voltages.shape
    n = n_chan * n_tm
    chips = n // 2
    channels = all_channels // n
    width = SUBLANES // parts
    groups = channels // width
    blocks = samples // FLAG_BLOCK_WIDTH
    segments = blocks * antennas
    most = 2 * segments
    levels = tuple(sorted({-(-most * step // LEVEL_STEPS[-1]) for step in LEVEL_STEPS}))
    dtype = voltages.dtype
    entries = segments + 1
    smem = pl.BlockSpec(memory_space=pltpu.SMEM)
    vmem = pl.BlockSpec(memory_space=pltpu.VMEM)
    hbm = pl.BlockSpec(memory_space=pltpu.HBM)
    first, rest, theirs, table, meta, level = pl.pallas_call(
        functools.partial(pack_kernel, n_chan, n_tm, levels),
        out_shape=(
            jax.ShapeDtypeStruct((2, chips, entries, SUBLANES, LANES), dtype),
            jax.ShapeDtypeStruct((chips, groups - 1, entries, SUBLANES, LANES), dtype),
            jax.ShapeDtypeStruct((chips, groups - 1, entries, SUBLANES, LANES), dtype),
            jax.ShapeDtypeStruct((n, LANES), jnp.int32),
            jax.ShapeDtypeStruct((2, n, LANES), jnp.int32),
            jax.ShapeDtypeStruct((1, LANES), jnp.int32),
        ),
        in_specs=[hbm, hbm, hbm],
        out_specs=(hbm, hbm, hbm, vmem, vmem, vmem),
        scratch_shapes=[
            pltpu.VMEM(voltages.shape, dtype),
            pltpu.VMEM((chips, groups, entries, SUBLANES, LANES), dtype),
            pltpu.VMEM((chips, groups, entries, SUBLANES, LANES), dtype),
            pltpu.VMEM((groups, SUBLANES * antennas, samples), jnp.float32),
            pltpu.VMEM((groups, SUBLANES * antennas, samples), jnp.float32),
            pltpu.VMEM((1, LANES), jnp.int32),
            pltpu.VMEM((n, 1, LANES), jnp.int32),
            pltpu.SMEM((2,) + flag_mask.shape, jnp.int32),
            pltpu.SMEM((3, segments), jnp.int32),
            pltpu.SemaphoreType.DMA((n,)),
            pltpu.SemaphoreType.DMA((2,)),
            pltpu.SemaphoreType.DMA((n,)),
            pltpu.SemaphoreType.DMA,
            pltpu.SemaphoreType.DMA,
            pltpu.SemaphoreType.DMA,
            pltpu.SemaphoreType.DMA((3,)),
        ],
        compiler_params=pltpu.CompilerParams(
            collective_id=0, has_side_effects=True, vmem_limit_bytes=67043328
        ),
    )(voltages, flag_mask, flagged_prefix_counts)
    total_antennas, total_samples = antennas * n_chan, samples * n_tm

    def unite(index, sent):
        return pl.pallas_call(
            functools.partial(unite_kernel, n_chan, n_tm, antennas, samples, sent),
            out_shape=jax.ShapeDtypeStruct((channels, 2, total_antennas, total_antennas), jnp.float32),
            in_specs=[hbm, hbm, hbm, vmem, smem],
            out_specs=hbm,
            scratch_shapes=[
                pltpu.VMEM((2, chips, entries, SUBLANES, LANES), dtype),
                pltpu.VMEM((2, chips, groups - 1, entries, SUBLANES, LANES), dtype),
                pltpu.VMEM((groups, chips, sent, SUBLANES, LANES), dtype),
                pltpu.VMEM((groups, chips, sent, SUBLANES, LANES), dtype),
                pltpu.VMEM((chips // BATCHES * (sent + 2), SUBLANES, LANES), jnp.float32),
                pltpu.VMEM((SUBLANES * antennas, samples), dtype),
                pltpu.VMEM((SUBLANES * antennas, samples), dtype),
                pltpu.VMEM((SUBLANES, total_antennas, total_samples), dtype),
                pltpu.VMEM((total_antennas, LANES), jnp.float32),
                pltpu.VMEM((total_antennas, total_antennas), jnp.float32),
                pltpu.VMEM((channels, 2, total_antennas, total_antennas), jnp.float32),
                pltpu.SemaphoreType.DMA((2,)),
                pltpu.SemaphoreType.DMA,
                pltpu.SemaphoreType.DMA,
                pltpu.SemaphoreType.DMA((groups, chips)),
                pltpu.SemaphoreType.DMA((groups, BATCHES)),
                pltpu.SemaphoreType.DMA((channels,)),
            ],
            compiler_params=pltpu.CompilerParams(
                collective_id=1 + index, has_side_effects=True, vmem_limit_bytes=48 * 1024 * 1024
            ),
        )

    branches = [unite(index, sent) for index, sent in enumerate(levels)]
    return lax.switch(level[0, 0], branches, first, rest, theirs, table, meta)


def packable(n_chan, n_tm, parts, all_channels, antennas, samples):
    n = n_chan * n_tm
    if n_chan % 2 or n // 2 % (2 * BATCHES) or all_channels % n or SUBLANES % parts:
        return False
    segments = samples // FLAG_BLOCK_WIDTH * antennas
    groups = all_channels // n // (SUBLANES // parts)
    return groups > 1 and all_channels == groups * n * (SUBLANES // parts) and antennas % 16 == 0 and segments < LANES - 1


def body(n_chan, n_tm, voltages, flag_mask, flagged_prefix_counts):
    chosen = packed_shards if packable(n_chan, n_tm, *voltages.shape) else shards
    return chosen(n_chan, n_tm, voltages, flag_mask, flagged_prefix_counts)


def solution(mesh):
    placed = (P(None, None, "chan", "tm"), P("tm", "chan"), P("tm", "chan"))
    return jax.shard_map(
        functools.partial(body, mesh.shape["chan"], mesh.shape["tm"]),
        mesh=mesh,
        in_specs=placed,
        out_specs=P(("chan", "tm"), None, None, None),
        check_vma=False,
    )
```

```python
import functools

import jax
import jax.numpy as jnp
from jax import lax
from jax.experimental import pallas as pl
from jax.experimental.pallas import tpu as pltpu
from jax.sharding import PartitionSpec as P

FLAG_BLOCK_WIDTH = 128
LANES = 128
SUBLANES = 8
AT, FIRST, LIMIT = 22, 15, 7
BATCHES = 8
LEVEL_STEPS = (8, 16, 22, 25, 26, 27, 28, 29, 30, 31, 32, 34, 38, 46, 64)
MESH = pl.DeviceIdType.MESH
NT = (((1,), (1,)), ((), ()))


def exchange_kernel(
    n_chan, n_tm, groups, volt_ref, limit_ref, out_ref,
    held, table, cols, keep, inverse, send_sem, recv_sem, table_send, table_recv,
):
    n = n_chan * n_tm
    channels = held.shape[1]
    step = channels // groups
    antennas, samples = volt_ref.shape[2], volt_ref.shape[3]
    total_antennas = n_chan * antennas
    local_blocks = samples // FLAG_BLOCK_WIDTH
    my_chan, my_tm = lax.axis_index("chan"), lax.axis_index("tm")
    me = my_chan * n_tm + my_tm

    def swing(m):
        return (m + 1) // 2 * (1 - 2 * lax.rem(m + 1, 2))

    def hop(k):
        return n // 2 + swing(k - 1)

    def place(k):
        other = lax.rem(me + hop(k), n)
        return other, (other // n_tm, lax.rem(other, n_tm))

    barrier = pltpu.get_barrier_semaphore()

    def greet(k, carry):
        pl.semaphore_signal(barrier, inc=1, device_id=place(k)[1], device_id_type=MESH)
        return carry

    lax.fori_loop(1, n, greet, 0)
    pl.semaphore_wait(barrier, n - 1)

    def landing(g):
        return held.at[
            :, pl.ds(g * step, step), my_chan, :, pl.ds(pl.multiple_of(my_tm * samples, LANES), samples)
        ]

    def flag_copy(k):
        return pltpu.make_async_remote_copy(
            src_ref=limit_ref, dst_ref=table.at[me], send_sem=table_send.at[k], recv_sem=table_recv,
            device_id=place(k)[1], device_id_type=MESH,
        )

    def volt_copy(g, k):
        other, where = place(k)
        return pltpu.make_async_remote_copy(
            src_ref=volt_ref.at[:, pl.ds(other * channels + g * step, step)],
            dst_ref=landing(g), send_sem=send_sem.at[g, k], recv_sem=recv_sem.at[g],
            device_id=where, device_id_type=MESH,
        )

    def each(body):
        def run(k, carry):
            body(k)
            return carry

        lax.fori_loop(1, n, run, 0)

    each(lambda k: flag_copy(k).start())
    for g in range(groups):
        each(lambda k, g=g: volt_copy(g, k).start())
    pltpu.make_async_copy(limit_ref, table.at[me], table_recv).start()
    for g in range(groups):
        pltpu.make_async_copy(
            volt_ref.at[:, pl.ds(me * channels + g * step, step)], landing(g), recv_sem.at[g]
        ).start()

    pltpu.make_async_copy(table, table, table_recv).wait()
    rows = table[:, 0, :].astype(jnp.float32)
    padding = -n % LANES
    if padding:
        rows = jnp.concatenate([rows, jnp.zeros((padding, rows.shape[1]), jnp.float32)], axis=0)
    turned = rows.T
    lane = lax.broadcasted_iota(jnp.int32, (total_antennas, LANES), 1).astype(jnp.float32)
    pairs = jnp.zeros((total_antennas, total_antennas), jnp.float32)
    for t in range(n_tm):
        for b in range(local_blocks):
            q = t * local_blocks + b
            for c in range(n_chan):
                source = c * n_tm + t
                cols[c * antennas:(c + 1) * antennas, :] = jnp.broadcast_to(
                    turned[b * antennas:(b + 1) * antennas, source:source + 1], (antennas, LANES)
                )
            column = cols[...]
            keep[:, q * LANES:(q + 1) * LANES] = jnp.where(lane >= column, 1.0, 0.0).astype(keep.dtype)
            pairs += FLAG_BLOCK_WIDTH - jnp.maximum(column[:, :1], column.T[:1, :])
    inverse[...] = 1.0 / jnp.maximum(pairs, 1.0)

    def correlate(c, carry):
        size = (total_antennas, keep.shape[1])
        real = held[0, c].reshape(size) * keep[...]
        imag = held[1, c].reshape(size) * keep[...]
        same = lax.dot_general(real, real, NT, preferred_element_type=jnp.float32)
        same += lax.dot_general(imag, imag, NT, preferred_element_type=jnp.float32)
        cross = lax.dot_general(imag, real, NT, preferred_element_type=jnp.float32)
        out_ref[c, 0] = same * inverse[...]
        out_ref[c, 1] = (cross - cross.T) * inverse[...]
        return carry

    for g in range(groups):
        part = held.at[:, pl.ds(g * step, step)]
        pltpu.make_async_copy(part, part, recv_sem.at[g]).wait()
        lax.fori_loop(g * step, (g + 1) * step, correlate, 0)

    each(lambda k: flag_copy(k).wait_send())
    for g in range(groups):
        each(lambda k, g=g: volt_copy(g, k).wait_send())


def shards(n_chan, n_tm, voltages, flag_mask, flagged_prefix_counts):
    parts, all_channels, antennas, samples = voltages.shape
    n = n_chan * n_tm
    channels = all_channels // n
    total_antennas, total_samples = antennas * n_chan, samples * n_tm
    groups = max(g for g in (4, 2, 1) if channels % g == 0)
    limits = jnp.where(flag_mask == 1, flagged_prefix_counts, FLAG_BLOCK_WIDTH).reshape(1, -1)
    limits = jnp.pad(limits, ((0, 0), (0, -limits.shape[1] % LANES)))
    width = limits.shape[1]
    return pl.pallas_call(
        functools.partial(exchange_kernel, n_chan, n_tm, groups),
        out_shape=pltpu.VMEM((channels, 2, total_antennas, total_antennas), jnp.float32),
        in_specs=[pl.BlockSpec(memory_space=pl.ANY), pl.BlockSpec(memory_space=pltpu.VMEM)],
        out_specs=pl.BlockSpec(memory_space=pltpu.VMEM),
        scratch_shapes=[
            pltpu.VMEM((parts, channels, n_chan, antennas, total_samples), voltages.dtype),
            pltpu.VMEM((n, 1, width), jnp.int32),
            pltpu.VMEM((total_antennas, LANES), jnp.float32),
            pltpu.VMEM((total_antennas, total_samples), voltages.dtype),
            pltpu.VMEM((total_antennas, total_antennas), jnp.float32),
            pltpu.SemaphoreType.DMA((groups, n)),
            pltpu.SemaphoreType.DMA((groups,)),
            pltpu.SemaphoreType.DMA((n,)),
            pltpu.SemaphoreType.DMA,
        ],
        compiler_params=pltpu.CompilerParams(
            collective_id=0, has_side_effects=True, vmem_limit_bytes=48 * 1024 * 1024
        ),
    )(voltages, limits)


def pack_kernel(
    n_chan, n_tm, levels, volt_ref, mask_ref, count_ref, first_ref, rest_ref, theirs_ref, table_ref, meta_ref, level_ref,
    held, theirs, mine, even, odd, row, table, flags, steps,
    load_sem, word_sem, flag_send, flag_recv, pair_send, pair_recv, keep_sem,
):
    n = n_chan * n_tm
    parts, all_channels, antennas, samples = volt_ref.shape
    channels = all_channels // n
    chips, groups = mine.shape[0], mine.shape[1]
    width = SUBLANES // parts
    blocks = samples // FLAG_BLOCK_WIDTH
    segments = blocks * antennas
    my_chan, my_tm = lax.axis_index("chan"), lax.axis_index("tm")
    me = my_chan * n_tm + my_tm
    side = lax.rem(my_chan, 2)
    partner = (my_chan + 1 - 2 * side, my_tm)

    def loop(low, high, do):
        def run(k, carry):
            do(k)
            return carry

        lax.fori_loop(low, high, run, 0)

    def others(do):
        def at(j, low):
            chan = my_chan + j
            chan = jnp.where(chan >= n_chan, chan - n_chan, chan)
            for u in range(low, n_tm):
                t = my_tm + u
                do(j * n_tm + u, (chan, jnp.where(t >= n_tm, t - n_tm, t)))

        loop(1, n_chan, lambda j: at(j, 0))
        at(0, 1)

    barrier = pltpu.get_barrier_semaphore()
    others(lambda k, where: pl.semaphore_signal(barrier, inc=1, device_id=where, device_id_type=MESH))
    words = [pltpu.make_async_copy(ref, flags.at[q], word_sem.at[q]) for q, ref in enumerate((mask_ref, count_ref))]
    for word in words:
        word.start()

    def load(d):
        part = pl.ds(d * channels, channels)
        return pltpu.make_async_copy(volt_ref.at[:, part], held.at[:, part], load_sem.at[d])

    def device_of(j):
        m = lax.rem(j, chips)
        chan = m // n_tm * 2 + lax.rem(side + 1 + j // chips, 2)
        return chan * n_tm + lax.rem(m, n_tm)

    loop(0, n, lambda j: load(device_of(j)).start())
    for word in words:
        word.wait()

    lane = lax.broadcasted_iota(jnp.int32, (SUBLANES, LANES), 1)
    limits = jnp.full((SUBLANES, LANES), FLAG_BLOCK_WIDTH, jnp.int32)
    total = jnp.int32(0)
    for s in range(segments):
        b, i = s // antennas, s % antennas
        flags[1, b, i] = jnp.where(flags[0, b, i] == 1, flags[1, b, i], FLAG_BLOCK_WIDTH)
        total = total + FLAG_BLOCK_WIDTH - flags[1, b, i]
    start = side * ((-total) & (LANES - 1))
    for s in range(segments):
        b, i = s // antennas, s % antennas
        limit = flags[1, b, i]
        limits = jnp.where(lane == s, limit, limits)
        first = start & (LANES - 1)
        spills = first + FLAG_BLOCK_WIDTH - limit > LANES
        steps[0, s] = (first - limit) & (LANES - 1)
        steps[1, s] = first
        steps[2, s] = jnp.where(spills, 0, first)
        start = start + FLAG_BLOCK_WIDTH - limit
    row[...] = limits[:1]

    old = lax.broadcasted_iota(jnp.int32, (SUBLANES * antennas, SUBLANES * antennas), 1)
    new = lax.broadcasted_iota(jnp.int32, (SUBLANES * antennas, SUBLANES * antennas), 0)
    turn = jnp.where(old == lax.rem(new, SUBLANES) * antennas + new // SUBLANES, 1.0, 0.0).astype(volt_ref.dtype)

    def flatten(j, flat):
        d = device_of(j)
        load(d).wait()
        for g in range(groups):
            part = held[:, pl.ds(d * channels + g * width, width)].reshape(SUBLANES * antennas, samples)
            flat[g] = jnp.dot(turn, part, preferred_element_type=jnp.float32)

    def merge(flat, target, m):
        carry = [jnp.zeros((SUBLANES, LANES), jnp.float32)] * groups
        for s in range(segments):
            b, i = s // antennas, s % antennas
            shift, opens, stays = steps[0, s], lane >= steps[1, s], lane >= steps[2, s]
            for g in range(groups):
                piece = flat[g, i * SUBLANES:(i + 1) * SUBLANES, b * LANES:(b + 1) * LANES]
                piece = pltpu.roll(piece, shift, axis=1)
                target[m, g, s] = jnp.where(opens, piece, carry[g]).astype(target.dtype)
                carry[g] = jnp.where(stays, piece, carry[g])
        for g in range(groups):
            target[m, g, segments] = carry[g].astype(target.dtype)

    def flag_copy(k, where):
        return pltpu.make_async_remote_copy(
            src_ref=row, dst_ref=table.at[me], send_sem=flag_send.at[k], recv_sem=flag_recv,
            device_id=where, device_id_type=MESH,
        )

    pair_copy = pltpu.make_async_remote_copy(
        src_ref=theirs.at[:, 0], dst_ref=first_ref.at[1], send_sem=pair_send, recv_sem=pair_recv,
        device_id=partner, device_id_type=MESH,
    )

    def keeps(h):
        part, later = pl.ds(2 * h, 2), pl.ds(1, groups - 1)
        return [
            pltpu.make_async_copy(ref, where, keep_sem.at[q, h])
            for q, (ref, where) in enumerate((
                (theirs.at[part, later], theirs_ref.at[part]),
                (mine.at[part, 0], first_ref.at[0, part]),
                (mine.at[part, later], rest_ref.at[part]),
            ))
        ]

    def keep_mine(h):
        for keep in keeps(h)[1:]:
            keep.start()

    def wait_keeps(h):
        for keep in keeps(h):
            keep.wait()

    def pack_theirs(h):
        flatten(2 * h + 1, odd)
        merge(even, theirs, 2 * h)
        flatten(2 * h + 2, even)
        merge(odd, theirs, 2 * h + 1)
        keeps(h)[0].start()

    def pack_mine(h):
        flatten(chips + 2 * h + 1, odd)
        merge(even, mine, 2 * h)
        flatten(chips + 2 * h + 2, even)
        merge(odd, mine, 2 * h + 1)
        keep_mine(h)

    flatten(0, even)
    early = chips * 5 // 16
    loop(0, early, pack_theirs)
    pl.semaphore_wait(barrier, n - 1)
    others(lambda k, where: flag_copy(k, where).start())
    loop(early, chips // 2, pack_theirs)
    pair_copy.start()
    pltpu.make_async_copy(row, table.at[me], flag_recv).start()
    loop(0, chips // 2 - 1, pack_mine)
    flatten(n - 1, odd)
    merge(even, mine, chips - 2)
    merge(odd, mine, chips - 1)
    keep_mine(chips // 2 - 1)

    pltpu.make_async_copy(table, table, flag_recv).wait()
    rows = table[:, 0, :]
    lanes = lax.broadcasted_iota(jnp.int32, (n, LANES), 1)
    kept = (FLAG_BLOCK_WIDTH - rows).astype(jnp.float32).astype(jnp.bfloat16)
    above = jnp.where(
        lax.broadcasted_iota(jnp.int32, (LANES, LANES), 0) < lax.broadcasted_iota(jnp.int32, (LANES, LANES), 1), 1.0, 0.0
    ).astype(jnp.bfloat16)
    offset = jnp.dot(kept, above, preferred_element_type=jnp.float32).astype(jnp.int32)
    total = jnp.broadcast_to(jnp.max(offset, axis=1, keepdims=True), (n, LANES))
    full = (total + (LANES - 1)) >> 7
    second = lax.rem(lax.broadcasted_iota(jnp.int32, (n, LANES), 0) // n_tm, 2) == 1
    offset = offset + jnp.where(second, (-total) & (LANES - 1), 0)
    to = lax.broadcasted_iota(jnp.int32, (n, n), 0)
    frm = lax.broadcasted_iota(jnp.int32, (n, n), 1)
    behind = jnp.where((frm == to - n_tm) & (lax.rem(to // n_tm, 2) == 1), 1.0, 0.0).astype(jnp.bfloat16)

    def fetch_behind(x):
        x = x.astype(jnp.float32).astype(jnp.bfloat16)
        return jnp.dot(behind, x, preferred_element_type=jnp.float32).astype(jnp.int32)

    ahead = (fetch_behind(total >> 7) << 7) + fetch_behind(total & (LANES - 1))
    pair = (total + ahead + (LANES - 1)) >> 7
    base = jnp.where(second, pair - full, 0)
    at = offset >> 7
    first = offset & (LANES - 1)
    meta_ref[0] = ((base + at) << AT) | (first << FIRST) | (rows << LIMIT) | ((rows - first) & (LANES - 1))
    place_of = jnp.full((n, LANES), -1, jnp.int32)
    for s in range(segments + 1):
        place_of += jnp.where(at[:, s:s + 1] <= lanes, 1, 0)
    place_of = jnp.where(lanes == LANES - 1, full, place_of)
    place_of = jnp.where(lanes == LANES - 2, base, place_of)
    meta_ref[1] = jnp.where(lanes == LANES - 3, total & (LANES - 1), place_of)
    table_ref[...] = rows
    need = jnp.max(pair, axis=0, keepdims=True)
    level = jnp.zeros((1, LANES), jnp.int32)
    for q in levels[:-1]:
        level += jnp.where(need > q, 1, 0)
    level_ref[...] = level

    loop(0, chips // 2, wait_keeps)
    pair_copy.wait()
    others(lambda k, where: flag_copy(k, where).wait_send())


def unite_kernel(
    n_chan, n_tm, antennas, samples, sent, first_ref, rest_ref, theirs_ref, table_ref, meta_ref, out_ref,
    first, rest, ready, landing, work, even, odd, square, cols, inverse,
    fetch_sem, pair_send, pair_recv, send_sem, recv_sem,
):
    groups = landing.shape[0]
    n, chips = n_chan * n_tm, first_ref.shape[1]
    half, batch = chips // 2, chips // recv_sem.shape[1]
    total_antennas, total_samples = square.shape[1], square.shape[2]
    blocks = samples // FLAG_BLOCK_WIDTH
    channels = out_ref.shape[0]
    width = channels // groups
    my_chan, my_tm = lax.axis_index("chan"), lax.axis_index("tm")
    side = lax.rem(my_chan, 2)
    here = my_chan // 2 * n_tm + my_tm
    my_half, my_place = here // half, lax.rem(here, half)
    partner = (my_chan + 1 - 2 * side, my_tm)

    def loop(low, high, do):
        def run(k, carry):
            do(k)
            return carry

        lax.fori_loop(low, high, run, 0)

    def chip_at(slot, step):
        other_half = lax.rem(my_half + slot // half, 2)
        return other_half * half + lax.rem(my_place + half + step * lax.rem(slot, half), half)

    def device_at(chip):
        return (chip // n_tm * 2 + side, lax.rem(chip, n_tm))

    barrier = pltpu.get_barrier_semaphore()
    loop(1, chips, lambda slot: pl.semaphore_signal(
        barrier, inc=1, device_id=device_at(chip_at(slot, 1)), device_id_type=MESH
    ))
    pl.semaphore_signal(barrier, inc=1, device_id=partner, device_id_type=MESH)
    fetches = [
        pltpu.make_async_copy(first_ref, first, fetch_sem.at[0]),
        pltpu.make_async_copy(rest_ref, rest.at[0], fetch_sem.at[1]),
    ]
    for fetch in fetches:
        fetch.start()
    pair_copy = pltpu.make_async_remote_copy(
        src_ref=theirs_ref, dst_ref=rest.at[1], send_sem=pair_send, recv_sem=pair_recv,
        device_id=partner, device_id_type=MESH,
    )
    low_device = (my_chan - side) * n_tm + my_tm
    high_device = low_device + n_tm
    low_rows, low_fill = meta_ref[1, low_device, LANES - 1], meta_ref[1, low_device, LANES - 3]
    high_base = meta_ref[1, high_device, LANES - 2]
    lanes = lax.broadcasted_iota(jnp.int32, (chips, SUBLANES, LANES), 2)

    def gather(g, source):
        def pick(r):
            low = source(side, meta_ref[1, low_device, r]).astype(jnp.float32)
            high = source(1 - side, meta_ref[1, high_device, jnp.maximum(r - high_base, 0)]).astype(jnp.float32)
            bound = jnp.where(r < high_base, LANES, jnp.where(r < low_rows, low_fill, 0))
            ready[g, :, r] = jnp.where(lanes < bound, low, high).astype(ready.dtype)

        loop(0, sent, pick)

    def copy(g, slot):
        chip = chip_at(slot, 1)
        return pltpu.make_async_remote_copy(
            src_ref=ready.at[g, chip], dst_ref=landing.at[g, slot, pl.ds(0, sent)],
            send_sem=send_sem.at[g, slot], recv_sem=recv_sem.at[g, slot // batch],
            device_id=device_at(chip), device_id_type=MESH,
        )

    def launch(g):
        loop(1, half, lambda slot: copy(g, slot).start())
        loop(0, half, lambda slot: copy(g, half + lax.rem(slot + half // 2, half)).start())
        pltpu.make_async_copy(ready.at[g, here], landing.at[g, 0, pl.ds(0, sent)], recv_sem.at[g, 0]).start()

    def gather_and_launch(g):
        gather(g, lambda w, entry: rest[w, :, g - 1, entry])
        launch(g)

    fetches[0].wait()
    gather(0, lambda w, entry: first[w, :, entry])
    pl.semaphore_wait(barrier, chips)
    pair_copy.start()
    launch(0)
    fetches[1].wait()
    pair_copy.wait_recv()
    loop(1, groups, gather_and_launch)

    rows = table_ref[...].astype(jnp.float32)
    padding = -n % LANES
    if padding:
        rows = jnp.concatenate([rows, jnp.zeros((padding, rows.shape[1]), jnp.float32)], axis=0)
    turned = rows.T
    pairs = jnp.zeros((total_antennas, total_antennas), jnp.float32)
    for t in range(n_tm):
        for b in range(blocks):
            for c in range(n_chan):
                source = c * n_tm + t
                cols[c * antennas:(c + 1) * antennas, :] = jnp.broadcast_to(
                    turned[b * antennas:(b + 1) * antennas, source:source + 1], (antennas, LANES)
                )
            column = cols[...]
            pairs += FLAG_BLOCK_WIDTH - jnp.maximum(column[:, :1], column.T[:1, :])
    inverse[...] = 1.0 / jnp.maximum(pairs, 1.0)

    lane = lax.broadcasted_iota(jnp.int32, (SUBLANES, LANES), 1)
    old = lax.broadcasted_iota(jnp.int32, (SUBLANES * antennas, SUBLANES * antennas), 1)
    new = lax.broadcasted_iota(jnp.int32, (SUBLANES * antennas, SUBLANES * antennas), 0)
    turn = jnp.where(new == lax.rem(old, SUBLANES) * antennas + old // SUBLANES, 1.0, 0.0).astype(square.dtype)

    lane_first = (lane << FIRST) | ((1 << FIRST) - 1)
    lane_limit = (lane << LIMIT) | ((1 << LIMIT) - 1)
    first_bits, limit_bits = (1 << AT) - (1 << FIRST), (1 << FIRST) - (1 << LIMIT)

    def source(part, q):
        chip = chip_at(part * batch + q // 2, -1)
        return chip // n_tm * 2 + lax.rem(q, 2), lax.rem(chip, n_tm)

    def expand(part, q, z):
        q = jnp.minimum(q, 2 * batch - 1)
        chan, t = source(part, q)
        d = chan * n_tm + t
        origin = q // 2 * (sent + 2)
        for i in range(antennas):
            for b in range(blocks):
                word = meta_ref[0, d, b * antennas + i]
                at = origin + (word >> AT)
                spread = jnp.full(lane.shape, word, jnp.int32)
                piece = jnp.where((spread & first_bits) <= lane_first, work[at], work[at + 1])
                piece = pltpu.roll(piece, word, axis=1)
                piece = jnp.where((spread & limit_bits) <= lane_limit, piece, 0.0)
                z[i * SUBLANES:(i + 1) * SUBLANES, b * LANES:(b + 1) * LANES] = piece.astype(z.dtype)

    def settle(part, q, z):
        chan, t = source(part, q)
        flat = jnp.dot(turn, z[...], preferred_element_type=jnp.float32).astype(square.dtype)
        for p in range(SUBLANES):
            square[
                p, pl.ds(pl.multiple_of(chan * antennas, antennas), antennas),
                pl.ds(pl.multiple_of(t * samples, LANES), samples),
            ] = flat[p * antennas:(p + 1) * antennas]

    def receive(g, part):
        arrived = landing.at[g, pl.ds(part * batch, batch), pl.ds(0, sent)]
        pltpu.make_async_copy(arrived, arrived, recv_sem.at[g, part]).wait()
        for j in range(batch):
            work[j * (sent + 2):j * (sent + 2) + sent] = landing[g, part * batch + j, :sent].astype(jnp.float32)
        expand(part, 0, even)

        def two(h):
            expand(part, 2 * h + 1, odd)
            settle(part, 2 * h, even)
            expand(part, 2 * h + 2, even)
            settle(part, 2 * h + 1, odd)

        loop(0, batch, two)

    def finish(g):
        loop(0, chips // batch, lambda part: receive(g, part))

        def correlate(c):
            real, imag = square[c], square[width + c]
            same = lax.dot_general(real, real, NT, preferred_element_type=jnp.float32)
            same += lax.dot_general(imag, imag, NT, preferred_element_type=jnp.float32)
            cross = lax.dot_general(imag, real, NT, preferred_element_type=jnp.float32)
            channel = g * width + c
            out_ref[channel, 0] = same * inverse[...]
            out_ref[channel, 1] = (cross - cross.T) * inverse[...]

        loop(0, width, correlate)

    loop(0, groups, finish)
    pair_copy.wait_send()
    loop(0, groups, lambda g: loop(1, chips, lambda slot: copy(g, slot).wait_send()))


def packed_shards(n_chan, n_tm, voltages, flag_mask, flagged_prefix_counts):
    parts, all_channels, antennas, samples = voltages.shape
    n = n_chan * n_tm
    chips = n // 2
    channels = all_channels // n
    width = SUBLANES // parts
    groups = channels // width
    blocks = samples // FLAG_BLOCK_WIDTH
    segments = blocks * antennas
    most = 2 * segments
    levels = tuple(sorted({-(-most * step // LEVEL_STEPS[-1]) for step in LEVEL_STEPS}))
    dtype = voltages.dtype
    entries = segments + 1
    smem = pl.BlockSpec(memory_space=pltpu.SMEM)
    vmem = pl.BlockSpec(memory_space=pltpu.VMEM)
    hbm = pl.BlockSpec(memory_space=pltpu.HBM)
    first, rest, theirs, table, meta, level = pl.pallas_call(
        functools.partial(pack_kernel, n_chan, n_tm, levels),
        out_shape=(
            jax.ShapeDtypeStruct((2, chips, entries, SUBLANES, LANES), dtype),
            jax.ShapeDtypeStruct((chips, groups - 1, entries, SUBLANES, LANES), dtype),
            jax.ShapeDtypeStruct((chips, groups - 1, entries, SUBLANES, LANES), dtype),
            jax.ShapeDtypeStruct((n, LANES), jnp.int32),
            jax.ShapeDtypeStruct((2, n, LANES), jnp.int32),
            jax.ShapeDtypeStruct((1, LANES), jnp.int32),
        ),
        in_specs=[hbm, hbm, hbm],
        out_specs=(hbm, hbm, hbm, vmem, vmem, vmem),
        scratch_shapes=[
            pltpu.VMEM(voltages.shape, dtype),
            pltpu.VMEM((chips, groups, entries, SUBLANES, LANES), dtype),
            pltpu.VMEM((chips, groups, entries, SUBLANES, LANES), dtype),
            pltpu.VMEM((groups, SUBLANES * antennas, samples), jnp.float32),
            pltpu.VMEM((groups, SUBLANES * antennas, samples), jnp.float32),
            pltpu.VMEM((1, LANES), jnp.int32),
            pltpu.VMEM((n, 1, LANES), jnp.int32),
            pltpu.SMEM((2,) + flag_mask.shape, jnp.int32),
            pltpu.SMEM((3, segments), jnp.int32),
            pltpu.SemaphoreType.DMA((n,)),
            pltpu.SemaphoreType.DMA((2,)),
            pltpu.SemaphoreType.DMA((n,)),
            pltpu.SemaphoreType.DMA,
            pltpu.SemaphoreType.DMA,
            pltpu.SemaphoreType.DMA,
            pltpu.SemaphoreType.DMA((3, chips // 2)),
        ],
        compiler_params=pltpu.CompilerParams(
            collective_id=0, has_side_effects=True, vmem_limit_bytes=67043328
        ),
    )(voltages, flag_mask, flagged_prefix_counts)
    total_antennas, total_samples = antennas * n_chan, samples * n_tm

    def unite(index, sent):
        return pl.pallas_call(
            functools.partial(unite_kernel, n_chan, n_tm, antennas, samples, sent),
            out_shape=pltpu.VMEM((channels, 2, total_antennas, total_antennas), jnp.float32),
            in_specs=[hbm, hbm, hbm, vmem, smem],
            out_specs=vmem,
            scratch_shapes=[
                pltpu.VMEM((2, chips, entries, SUBLANES, LANES), dtype),
                pltpu.VMEM((2, chips, groups - 1, entries, SUBLANES, LANES), dtype),
                pltpu.VMEM((groups, chips, sent, SUBLANES, LANES), dtype),
                pltpu.VMEM((groups, chips, sent, SUBLANES, LANES), dtype),
                pltpu.VMEM((chips // BATCHES * (sent + 2), SUBLANES, LANES), jnp.float32),
                pltpu.VMEM((SUBLANES * antennas, samples), dtype),
                pltpu.VMEM((SUBLANES * antennas, samples), dtype),
                pltpu.VMEM((SUBLANES, total_antennas, total_samples), dtype),
                pltpu.VMEM((total_antennas, LANES), jnp.float32),
                pltpu.VMEM((total_antennas, total_antennas), jnp.float32),
                pltpu.SemaphoreType.DMA((2,)),
                pltpu.SemaphoreType.DMA,
                pltpu.SemaphoreType.DMA,
                pltpu.SemaphoreType.DMA((groups, chips)),
                pltpu.SemaphoreType.DMA((groups, BATCHES)),
            ],
            compiler_params=pltpu.CompilerParams(
                collective_id=1 + index, has_side_effects=True, vmem_limit_bytes=48 * 1024 * 1024
            ),
        )

    branches = [unite(index, sent) for index, sent in enumerate(levels)]
    return lax.switch(level[0, 0], branches, first, rest, theirs, table, meta)


def packable(n_chan, n_tm, parts, all_channels, antennas, samples):
    n = n_chan * n_tm
    if n_chan % 2 or n // 2 % (2 * BATCHES) or all_channels % n or SUBLANES % parts:
        return False
    segments = samples // FLAG_BLOCK_WIDTH * antennas
    groups = all_channels // n // (SUBLANES // parts)
    return groups > 1 and all_channels == groups * n * (SUBLANES // parts) and antennas % 16 == 0 and segments * 2 < LANES - 3


def body(n_chan, n_tm, voltages, flag_mask, flagged_prefix_counts):
    chosen = packed_shards if packable(n_chan, n_tm, *voltages.shape) else shards
    return chosen(n_chan, n_tm, voltages, flag_mask, flagged_prefix_counts)


def solution(mesh):
    placed = (P(None, None, "chan", "tm"), P("tm", "chan"), P("tm", "chan"))
    return jax.shard_map(
        functools.partial(body, mesh.shape["chan"], mesh.shape["tm"]),
        mesh=mesh,
        in_specs=placed,
        out_specs=P(("chan", "tm"), None, None, None),
        check_vma=False,
    )
```

```python
import functools

import jax
import jax.numpy as jnp
from jax import lax
from jax.experimental import pallas as pl
from jax.experimental.pallas import tpu as pltpu
from jax.sharding import PartitionSpec as P

FLAG_BLOCK_WIDTH = 128
LANES = 128
SUBLANES = 8
AT, FIRST, LIMIT = 22, 15, 7
BATCHES = 8
LEVEL_STEPS = (8, 16, 22, 25, 26, 27, 28, 29, 30, 31, 32, 34, 38, 46, 64)
MESH = pl.DeviceIdType.MESH
NT = (((1,), (1,)), ((), ()))


def exchange_kernel(
    n_chan, n_tm, groups, volt_ref, limit_ref, out_ref,
    held, table, cols, keep, inverse, send_sem, recv_sem, table_send, table_recv,
):
    n = n_chan * n_tm
    channels = held.shape[1]
    step = channels // groups
    antennas, samples = volt_ref.shape[2], volt_ref.shape[3]
    total_antennas = n_chan * antennas
    local_blocks = samples // FLAG_BLOCK_WIDTH
    my_chan, my_tm = lax.axis_index("chan"), lax.axis_index("tm")
    me = my_chan * n_tm + my_tm

    def swing(m):
        return (m + 1) // 2 * (1 - 2 * lax.rem(m + 1, 2))

    def hop(k):
        return n // 2 + swing(k - 1)

    def place(k):
        other = lax.rem(me + hop(k), n)
        return other, (other // n_tm, lax.rem(other, n_tm))

    barrier = pltpu.get_barrier_semaphore()

    def greet(k, carry):
        pl.semaphore_signal(barrier, inc=1, device_id=place(k)[1], device_id_type=MESH)
        return carry

    lax.fori_loop(1, n, greet, 0)
    pl.semaphore_wait(barrier, n - 1)

    def landing(g):
        return held.at[
            :, pl.ds(g * step, step), my_chan, :, pl.ds(pl.multiple_of(my_tm * samples, LANES), samples)
        ]

    def flag_copy(k):
        return pltpu.make_async_remote_copy(
            src_ref=limit_ref, dst_ref=table.at[me], send_sem=table_send.at[k], recv_sem=table_recv,
            device_id=place(k)[1], device_id_type=MESH,
        )

    def volt_copy(g, k):
        other, where = place(k)
        return pltpu.make_async_remote_copy(
            src_ref=volt_ref.at[:, pl.ds(other * channels + g * step, step)],
            dst_ref=landing(g), send_sem=send_sem.at[g, k], recv_sem=recv_sem.at[g],
            device_id=where, device_id_type=MESH,
        )

    def each(body):
        def run(k, carry):
            body(k)
            return carry

        lax.fori_loop(1, n, run, 0)

    each(lambda k: flag_copy(k).start())
    for g in range(groups):
        each(lambda k, g=g: volt_copy(g, k).start())
    pltpu.make_async_copy(limit_ref, table.at[me], table_recv).start()
    for g in range(groups):
        pltpu.make_async_copy(
            volt_ref.at[:, pl.ds(me * channels + g * step, step)], landing(g), recv_sem.at[g]
        ).start()

    pltpu.make_async_copy(table, table, table_recv).wait()
    rows = table[:, 0, :].astype(jnp.float32)
    padding = -n % LANES
    if padding:
        rows = jnp.concatenate([rows, jnp.zeros((padding, rows.shape[1]), jnp.float32)], axis=0)
    turned = rows.T
    lane = lax.broadcasted_iota(jnp.int32, (total_antennas, LANES), 1).astype(jnp.float32)
    pairs = jnp.zeros((total_antennas, total_antennas), jnp.float32)
    for t in range(n_tm):
        for b in range(local_blocks):
            q = t * local_blocks + b
            for c in range(n_chan):
                source = c * n_tm + t
                cols[c * antennas:(c + 1) * antennas, :] = jnp.broadcast_to(
                    turned[b * antennas:(b + 1) * antennas, source:source + 1], (antennas, LANES)
                )
            column = cols[...]
            keep[:, q * LANES:(q + 1) * LANES] = jnp.where(lane >= column, 1.0, 0.0).astype(keep.dtype)
            pairs += FLAG_BLOCK_WIDTH - jnp.maximum(column[:, :1], column.T[:1, :])
    inverse[...] = 1.0 / jnp.maximum(pairs, 1.0)

    def correlate(c, carry):
        size = (total_antennas, keep.shape[1])
        real = held[0, c].reshape(size) * keep[...]
        imag = held[1, c].reshape(size) * keep[...]
        same = lax.dot_general(real, real, NT, preferred_element_type=jnp.float32)
        same += lax.dot_general(imag, imag, NT, preferred_element_type=jnp.float32)
        cross = lax.dot_general(imag, real, NT, preferred_element_type=jnp.float32)
        out_ref[c, 0] = same * inverse[...]
        out_ref[c, 1] = (cross - cross.T) * inverse[...]
        return carry

    for g in range(groups):
        part = held.at[:, pl.ds(g * step, step)]
        pltpu.make_async_copy(part, part, recv_sem.at[g]).wait()
        lax.fori_loop(g * step, (g + 1) * step, correlate, 0)

    each(lambda k: flag_copy(k).wait_send())
    for g in range(groups):
        each(lambda k, g=g: volt_copy(g, k).wait_send())


def shards(n_chan, n_tm, voltages, flag_mask, flagged_prefix_counts):
    parts, all_channels, antennas, samples = voltages.shape
    n = n_chan * n_tm
    channels = all_channels // n
    total_antennas, total_samples = antennas * n_chan, samples * n_tm
    groups = max(g for g in (4, 2, 1) if channels % g == 0)
    limits = jnp.where(flag_mask == 1, flagged_prefix_counts, FLAG_BLOCK_WIDTH).reshape(1, -1)
    limits = jnp.pad(limits, ((0, 0), (0, -limits.shape[1] % LANES)))
    width = limits.shape[1]
    return pl.pallas_call(
        functools.partial(exchange_kernel, n_chan, n_tm, groups),
        out_shape=pltpu.VMEM((channels, 2, total_antennas, total_antennas), jnp.float32),
        in_specs=[pl.BlockSpec(memory_space=pl.ANY), pl.BlockSpec(memory_space=pltpu.VMEM)],
        out_specs=pl.BlockSpec(memory_space=pltpu.VMEM),
        scratch_shapes=[
            pltpu.VMEM((parts, channels, n_chan, antennas, total_samples), voltages.dtype),
            pltpu.VMEM((n, 1, width), jnp.int32),
            pltpu.VMEM((total_antennas, LANES), jnp.float32),
            pltpu.VMEM((total_antennas, total_samples), voltages.dtype),
            pltpu.VMEM((total_antennas, total_antennas), jnp.float32),
            pltpu.SemaphoreType.DMA((groups, n)),
            pltpu.SemaphoreType.DMA((groups,)),
            pltpu.SemaphoreType.DMA((n,)),
            pltpu.SemaphoreType.DMA,
        ],
        compiler_params=pltpu.CompilerParams(
            collective_id=0, has_side_effects=True, vmem_limit_bytes=48 * 1024 * 1024
        ),
    )(voltages, limits)


def pack_kernel(
    n_chan, n_tm, levels, volt_ref, mask_ref, count_ref, first_ref, rest_ref, theirs_ref, table_ref, meta_ref, level_ref,
    held, theirs, mine, even, odd, row, table, flags, steps,
    load_sem, word_sem, flag_send, flag_recv, pair_send, pair_recv, keep_sem,
):
    n = n_chan * n_tm
    parts, all_channels, antennas, samples = volt_ref.shape
    channels = all_channels // n
    chips, groups = mine.shape[0], mine.shape[1]
    width = SUBLANES // parts
    blocks = samples // FLAG_BLOCK_WIDTH
    segments = blocks * antennas
    my_chan, my_tm = lax.axis_index("chan"), lax.axis_index("tm")
    me = my_chan * n_tm + my_tm
    side = lax.rem(my_chan, 2)
    partner = (my_chan + 1 - 2 * side, my_tm)

    def loop(low, high, do):
        def run(k, carry):
            do(k)
            return carry

        lax.fori_loop(low, high, run, 0)

    def others(do):
        def at(j, low):
            chan = my_chan + j
            chan = jnp.where(chan >= n_chan, chan - n_chan, chan)
            for u in range(low, n_tm):
                t = my_tm + u
                do(j * n_tm + u, (chan, jnp.where(t >= n_tm, t - n_tm, t)))

        loop(1, n_chan, lambda j: at(j, 0))
        at(0, 1)

    barrier = pltpu.get_barrier_semaphore()
    others(lambda k, where: pl.semaphore_signal(barrier, inc=1, device_id=where, device_id_type=MESH))
    words = [pltpu.make_async_copy(ref, flags.at[q], word_sem.at[q]) for q, ref in enumerate((mask_ref, count_ref))]
    for word in words:
        word.start()

    def load(d):
        part = pl.ds(d * channels, channels)
        return pltpu.make_async_copy(volt_ref.at[:, part], held.at[:, part], load_sem.at[d])

    def device_of(j):
        m = lax.rem(j, chips)
        chan = m // n_tm * 2 + lax.rem(side + 1 + j // chips, 2)
        return chan * n_tm + lax.rem(m, n_tm)

    loop(0, n, lambda j: load(device_of(j)).start())
    for word in words:
        word.wait()

    lane = lax.broadcasted_iota(jnp.int32, (SUBLANES, LANES), 1)
    limits = jnp.full((SUBLANES, LANES), FLAG_BLOCK_WIDTH, jnp.int32)
    total = jnp.int32(0)
    for s in range(segments):
        b, i = s // antennas, s % antennas
        flags[1, b, i] = jnp.where(flags[0, b, i] == 1, flags[1, b, i], FLAG_BLOCK_WIDTH)
        total = total + FLAG_BLOCK_WIDTH - flags[1, b, i]
    start = side * ((-total) & (LANES - 1))
    for s in range(segments):
        b, i = s // antennas, s % antennas
        limit = flags[1, b, i]
        limits = jnp.where(lane == s, limit, limits)
        first = start & (LANES - 1)
        spills = first + FLAG_BLOCK_WIDTH - limit > LANES
        steps[0, s] = (first - limit) & (LANES - 1)
        steps[1, s] = first
        steps[2, s] = jnp.where(spills, 0, first)
        start = start + FLAG_BLOCK_WIDTH - limit
    row[...] = limits[:1]

    old = lax.broadcasted_iota(jnp.int32, (SUBLANES * antennas, SUBLANES * antennas), 1)
    new = lax.broadcasted_iota(jnp.int32, (SUBLANES * antennas, SUBLANES * antennas), 0)
    turn = jnp.where(old == lax.rem(new, SUBLANES) * antennas + new // SUBLANES, 1.0, 0.0).astype(volt_ref.dtype)

    def flatten(j, flat):
        d = device_of(j)
        load(d).wait()
        for g in range(groups):
            part = held[:, pl.ds(d * channels + g * width, width)].reshape(SUBLANES * antennas, samples)
            flat[g] = jnp.dot(turn, part, preferred_element_type=jnp.float32)

    def merge(flat, target, m):
        carry = [jnp.zeros((SUBLANES, LANES), jnp.float32)] * groups
        for s in range(segments):
            b, i = s // antennas, s % antennas
            shift, opens, stays = steps[0, s], lane >= steps[1, s], lane >= steps[2, s]
            for g in range(groups):
                piece = flat[g, i * SUBLANES:(i + 1) * SUBLANES, b * LANES:(b + 1) * LANES]
                piece = pltpu.roll(piece, shift, axis=1)
                target[m, g, s] = jnp.where(opens, piece, carry[g]).astype(target.dtype)
                carry[g] = jnp.where(stays, piece, carry[g])
        for g in range(groups):
            target[m, g, segments] = carry[g].astype(target.dtype)

    def flag_copy(k, where):
        return pltpu.make_async_remote_copy(
            src_ref=row, dst_ref=table.at[me], send_sem=flag_send.at[k], recv_sem=flag_recv,
            device_id=where, device_id_type=MESH,
        )

    pair_copy = pltpu.make_async_remote_copy(
        src_ref=theirs.at[:, 0], dst_ref=first_ref.at[1], send_sem=pair_send, recv_sem=pair_recv,
        device_id=partner, device_id_type=MESH,
    )

    def keeps(h):
        part, later = pl.ds(2 * h, 2), pl.ds(1, groups - 1)
        return [
            pltpu.make_async_copy(ref, where, keep_sem.at[q, h])
            for q, (ref, where) in enumerate((
                (theirs.at[part, later], theirs_ref.at[part]),
                (mine.at[part, 0], first_ref.at[0, part]),
                (mine.at[part, later], rest_ref.at[part]),
            ))
        ]

    def keep_mine(h):
        for keep in keeps(h)[1:]:
            keep.start()

    def wait_keeps(h):
        for keep in keeps(h):
            keep.wait()

    def pack_theirs(h):
        flatten(2 * h + 1, odd)
        merge(even, theirs, 2 * h)
        flatten(2 * h + 2, even)
        merge(odd, theirs, 2 * h + 1)
        keeps(h)[0].start()

    def pack_mine(h):
        flatten(chips + 2 * h + 1, odd)
        merge(even, mine, 2 * h)
        flatten(chips + 2 * h + 2, even)
        merge(odd, mine, 2 * h + 1)
        keep_mine(h)

    flatten(0, even)
    early = chips * 5 // 16
    loop(0, early, pack_theirs)
    pl.semaphore_wait(barrier, n - 1)
    others(lambda k, where: flag_copy(k, where).start())
    loop(early, chips // 2, pack_theirs)
    pair_copy.start()
    pltpu.make_async_copy(row, table.at[me], flag_recv).start()
    loop(0, chips // 2 - 1, pack_mine)
    flatten(n - 1, odd)
    merge(even, mine, chips - 2)
    merge(odd, mine, chips - 1)
    keep_mine(chips // 2 - 1)

    pltpu.make_async_copy(table, table, flag_recv).wait()
    rows = table[:, 0, :]
    lanes = lax.broadcasted_iota(jnp.int32, (n, LANES), 1)
    kept = (FLAG_BLOCK_WIDTH - rows).astype(jnp.float32).astype(jnp.bfloat16)
    above = jnp.where(
        lax.broadcasted_iota(jnp.int32, (LANES, LANES), 0) < lax.broadcasted_iota(jnp.int32, (LANES, LANES), 1), 1.0, 0.0
    ).astype(jnp.bfloat16)
    offset = jnp.dot(kept, above, preferred_element_type=jnp.float32).astype(jnp.int32)
    total = jnp.broadcast_to(jnp.max(offset, axis=1, keepdims=True), (n, LANES))
    full = (total + (LANES - 1)) >> 7
    second = lax.rem(lax.broadcasted_iota(jnp.int32, (n, LANES), 0) // n_tm, 2) == 1
    offset = offset + jnp.where(second, (-total) & (LANES - 1), 0)
    to = lax.broadcasted_iota(jnp.int32, (n, n), 0)
    frm = lax.broadcasted_iota(jnp.int32, (n, n), 1)
    behind = jnp.where((frm == to - n_tm) & (lax.rem(to // n_tm, 2) == 1), 1.0, 0.0).astype(jnp.bfloat16)

    def fetch_behind(x):
        x = x.astype(jnp.float32).astype(jnp.bfloat16)
        return jnp.dot(behind, x, preferred_element_type=jnp.float32).astype(jnp.int32)

    ahead = (fetch_behind(total >> 7) << 7) + fetch_behind(total & (LANES - 1))
    pair = (total + ahead + (LANES - 1)) >> 7
    base = jnp.where(second, pair - full, 0)
    at = offset >> 7
    first = offset & (LANES - 1)
    meta_ref[0] = ((base + at) << AT) | (first << FIRST) | (rows << LIMIT) | ((rows - first) & (LANES - 1))
    place_of = jnp.full((n, LANES), -1, jnp.int32)
    for s in range(segments + 1):
        place_of += jnp.where(at[:, s:s + 1] <= lanes, 1, 0)
    place_of = jnp.where(lanes == LANES - 1, full, place_of)
    place_of = jnp.where(lanes == LANES - 2, base, place_of)
    meta_ref[1] = jnp.where(lanes == LANES - 3, total & (LANES - 1), place_of)
    table_ref[...] = rows
    need = jnp.max(pair, axis=0, keepdims=True)
    level = jnp.zeros((1, LANES), jnp.int32)
    for q in levels[:-1]:
        level += jnp.where(need > q, 1, 0)
    level_ref[...] = level

    loop(0, chips // 2, wait_keeps)
    pair_copy.wait()
    others(lambda k, where: flag_copy(k, where).wait_send())


def unite_kernel(
    n_chan, n_tm, antennas, samples, sent, first_ref, rest_ref, theirs_ref, table_hbm, meta_hbm, out_ref,
    table_ref, meta_ref, first, rest, ready, landing, work, even, odd, square, cols, inverse,
    fetch_sem, pair_send, pair_recv, send_sem, recv_sem,
):
    groups = landing.shape[0]
    n, chips = n_chan * n_tm, first_ref.shape[1]
    half, batch = chips // 2, chips // recv_sem.shape[1]
    total_antennas, total_samples = square.shape[1], square.shape[2]
    blocks = samples // FLAG_BLOCK_WIDTH
    channels = out_ref.shape[0]
    width = channels // groups
    my_chan, my_tm = lax.axis_index("chan"), lax.axis_index("tm")
    side = lax.rem(my_chan, 2)
    here = my_chan // 2 * n_tm + my_tm
    my_half, my_place = here // half, lax.rem(here, half)
    partner = (my_chan + 1 - 2 * side, my_tm)

    def loop(low, high, do):
        def run(k, carry):
            do(k)
            return carry

        lax.fori_loop(low, high, run, 0)

    def chip_at(slot, step):
        other_half = lax.rem(my_half + slot // half, 2)
        return other_half * half + lax.rem(my_place + half + step * lax.rem(slot, half), half)

    def device_at(chip):
        return (chip // n_tm * 2 + side, lax.rem(chip, n_tm))

    barrier = pltpu.get_barrier_semaphore()
    loop(1, chips, lambda k: pl.semaphore_signal(
        barrier, inc=1, device_id=device_at(lax.rem(here + k, chips)), device_id_type=MESH
    ))
    pl.semaphore_signal(barrier, inc=1, device_id=partner, device_id_type=MESH)
    fetches = [
        pltpu.make_async_copy(first_ref, first, fetch_sem.at[0]),
        pltpu.make_async_copy(rest_ref, rest.at[0], fetch_sem.at[1]),
        pltpu.make_async_copy(meta_hbm, meta_ref, fetch_sem.at[2]),
        pltpu.make_async_copy(table_hbm, table_ref, fetch_sem.at[3]),
    ]
    for q in (2, 0, 3, 1):
        fetches[q].start()
    pair_copy = pltpu.make_async_remote_copy(
        src_ref=theirs_ref, dst_ref=rest.at[1], send_sem=pair_send, recv_sem=pair_recv,
        device_id=partner, device_id_type=MESH,
    )
    fetches[2].wait()
    low_device = (my_chan - side) * n_tm + my_tm
    high_device = low_device + n_tm
    low_rows, low_fill = meta_ref[1, low_device, LANES - 1], meta_ref[1, low_device, LANES - 3]
    high_base = meta_ref[1, high_device, LANES - 2]
    lanes = lax.broadcasted_iota(jnp.int32, (chips, SUBLANES, LANES), 2)

    def gather(g, source):
        def pick(r):
            low = source(side, meta_ref[1, low_device, r]).astype(jnp.float32)
            high = source(1 - side, meta_ref[1, high_device, jnp.maximum(r - high_base, 0)]).astype(jnp.float32)
            bound = jnp.where(r < high_base, LANES, jnp.where(r < low_rows, low_fill, 0))
            ready[g, :, r] = jnp.where(lanes < bound, low, high).astype(ready.dtype)

        loop(0, sent, pick)

    def copy(g, slot):
        chip = chip_at(slot, 1)
        return pltpu.make_async_remote_copy(
            src_ref=ready.at[g, chip], dst_ref=landing.at[g, slot, pl.ds(0, sent)],
            send_sem=send_sem.at[g, slot], recv_sem=recv_sem.at[g, slot // batch],
            device_id=device_at(chip), device_id_type=MESH,
        )

    def launch(g):
        loop(1, half, lambda slot: copy(g, slot).start())
        loop(0, half, lambda slot: copy(g, half + lax.rem(slot + half // 2, half)).start())
        pltpu.make_async_copy(ready.at[g, here], landing.at[g, 0, pl.ds(0, sent)], recv_sem.at[g, 0]).start()

    def gather_and_launch(g):
        gather(g, lambda w, entry: rest[w, :, g - 1, entry])
        launch(g)

    fetches[0].wait()
    gather(0, lambda w, entry: first[w, :, entry])
    pl.semaphore_wait(barrier, chips)
    pair_copy.start()
    launch(0)
    fetches[1].wait()
    pair_copy.wait_recv()
    loop(1, groups, gather_and_launch)

    fetches[3].wait()
    rows = table_ref[...].astype(jnp.float32)
    padding = -n % LANES
    if padding:
        rows = jnp.concatenate([rows, jnp.zeros((padding, rows.shape[1]), jnp.float32)], axis=0)
    turned = rows.T
    pairs = jnp.zeros((total_antennas, total_antennas), jnp.float32)
    for t in range(n_tm):
        for b in range(blocks):
            for c in range(n_chan):
                source = c * n_tm + t
                cols[c * antennas:(c + 1) * antennas, :] = jnp.broadcast_to(
                    turned[b * antennas:(b + 1) * antennas, source:source + 1], (antennas, LANES)
                )
            column = cols[...]
            pairs += FLAG_BLOCK_WIDTH - jnp.maximum(column[:, :1], column.T[:1, :])
    inverse[...] = 1.0 / jnp.maximum(pairs, 1.0)

    lane = lax.broadcasted_iota(jnp.int32, (SUBLANES, LANES), 1)
    old = lax.broadcasted_iota(jnp.int32, (SUBLANES * antennas, SUBLANES * antennas), 1)
    new = lax.broadcasted_iota(jnp.int32, (SUBLANES * antennas, SUBLANES * antennas), 0)
    turn = jnp.where(new == lax.rem(old, SUBLANES) * antennas + old // SUBLANES, 1.0, 0.0).astype(square.dtype)

    lane_first = (lane << FIRST) | ((1 << FIRST) - 1)
    lane_limit = (lane << LIMIT) | ((1 << LIMIT) - 1)
    first_bits, limit_bits = (1 << AT) - (1 << FIRST), (1 << FIRST) - (1 << LIMIT)

    def source(part, q):
        chip = chip_at(part * batch + q // 2, -1)
        return chip // n_tm * 2 + lax.rem(q, 2), lax.rem(chip, n_tm)

    def expand(part, q, z):
        q = jnp.minimum(q, 2 * batch - 1)
        chan, t = source(part, q)
        d = chan * n_tm + t
        origin = q // 2 * (sent + 2)
        for i in range(antennas):
            for b in range(blocks):
                word = meta_ref[0, d, b * antennas + i]
                at = origin + (word >> AT)
                spread = jnp.full(lane.shape, word, jnp.int32)
                piece = jnp.where((spread & first_bits) <= lane_first, work[at], work[at + 1])
                piece = pltpu.roll(piece, word, axis=1)
                piece = jnp.where((spread & limit_bits) <= lane_limit, piece, 0.0)
                z[i * SUBLANES:(i + 1) * SUBLANES, b * LANES:(b + 1) * LANES] = piece.astype(z.dtype)

    def settle(part, q, z):
        chan, t = source(part, q)
        flat = jnp.dot(turn, z[...], preferred_element_type=jnp.float32).astype(square.dtype)
        for p in range(SUBLANES):
            square[
                p, pl.ds(pl.multiple_of(chan * antennas, antennas), antennas),
                pl.ds(pl.multiple_of(t * samples, LANES), samples),
            ] = flat[p * antennas:(p + 1) * antennas]

    def receive(g, part):
        arrived = landing.at[g, pl.ds(part * batch, batch), pl.ds(0, sent)]
        pltpu.make_async_copy(arrived, arrived, recv_sem.at[g, part]).wait()
        for j in range(batch):
            work[j * (sent + 2):j * (sent + 2) + sent] = landing[g, part * batch + j, :sent].astype(jnp.float32)
        expand(part, 0, even)

        def two(h):
            expand(part, 2 * h + 1, odd)
            settle(part, 2 * h, even)
            expand(part, 2 * h + 2, even)
            settle(part, 2 * h + 1, odd)

        loop(0, batch, two)

    def finish(g):
        loop(0, chips // batch, lambda part: receive(g, part))

        def correlate(c):
            real, imag = square[c], square[width + c]
            same = lax.dot_general(real, real, NT, preferred_element_type=jnp.float32)
            same += lax.dot_general(imag, imag, NT, preferred_element_type=jnp.float32)
            cross = lax.dot_general(imag, real, NT, preferred_element_type=jnp.float32)
            channel = g * width + c
            out_ref[channel, 0] = same * inverse[...]
            out_ref[channel, 1] = (cross - cross.T) * inverse[...]

        loop(0, width, correlate)

    loop(0, groups, finish)
    pair_copy.wait_send()
    loop(0, groups, lambda g: loop(1, chips, lambda slot: copy(g, slot).wait_send()))


def packed_shards(n_chan, n_tm, voltages, flag_mask, flagged_prefix_counts):
    parts, all_channels, antennas, samples = voltages.shape
    n = n_chan * n_tm
    chips = n // 2
    channels = all_channels // n
    width = SUBLANES // parts
    groups = channels // width
    blocks = samples // FLAG_BLOCK_WIDTH
    segments = blocks * antennas
    most = 2 * segments
    levels = tuple(sorted({-(-most * step // LEVEL_STEPS[-1]) for step in LEVEL_STEPS}))
    dtype = voltages.dtype
    entries = segments + 1
    vmem = pl.BlockSpec(memory_space=pltpu.VMEM)
    hbm = pl.BlockSpec(memory_space=pltpu.HBM)
    first, rest, theirs, table, meta, level = pl.pallas_call(
        functools.partial(pack_kernel, n_chan, n_tm, levels),
        out_shape=(
            jax.ShapeDtypeStruct((2, chips, entries, SUBLANES, LANES), dtype),
            jax.ShapeDtypeStruct((chips, groups - 1, entries, SUBLANES, LANES), dtype),
            jax.ShapeDtypeStruct((chips, groups - 1, entries, SUBLANES, LANES), dtype),
            jax.ShapeDtypeStruct((n, LANES), jnp.int32),
            jax.ShapeDtypeStruct((2, n, LANES), jnp.int32),
            jax.ShapeDtypeStruct((1, LANES), jnp.int32),
        ),
        in_specs=[hbm, hbm, hbm],
        out_specs=(hbm, hbm, hbm, vmem, vmem, vmem),
        scratch_shapes=[
            pltpu.VMEM(voltages.shape, dtype),
            pltpu.VMEM((chips, groups, entries, SUBLANES, LANES), dtype),
            pltpu.VMEM((chips, groups, entries, SUBLANES, LANES), dtype),
            pltpu.VMEM((groups, SUBLANES * antennas, samples), jnp.float32),
            pltpu.VMEM((groups, SUBLANES * antennas, samples), jnp.float32),
            pltpu.VMEM((1, LANES), jnp.int32),
            pltpu.VMEM((n, 1, LANES), jnp.int32),
            pltpu.SMEM((2,) + flag_mask.shape, jnp.int32),
            pltpu.SMEM((3, segments), jnp.int32),
            pltpu.SemaphoreType.DMA((n,)),
            pltpu.SemaphoreType.DMA((2,)),
            pltpu.SemaphoreType.DMA((n,)),
            pltpu.SemaphoreType.DMA,
            pltpu.SemaphoreType.DMA,
            pltpu.SemaphoreType.DMA,
            pltpu.SemaphoreType.DMA((3, chips // 2)),
        ],
        compiler_params=pltpu.CompilerParams(
            collective_id=0, has_side_effects=True, vmem_limit_bytes=67043328
        ),
    )(voltages, flag_mask, flagged_prefix_counts)
    total_antennas, total_samples = antennas * n_chan, samples * n_tm

    def unite(index, sent):
        return pl.pallas_call(
            functools.partial(unite_kernel, n_chan, n_tm, antennas, samples, sent),
            out_shape=pltpu.VMEM((channels, 2, total_antennas, total_antennas), jnp.float32),
            in_specs=[hbm] * 5,
            out_specs=vmem,
            scratch_shapes=[
                pltpu.VMEM((n, LANES), jnp.int32),
                pltpu.SMEM((2, n, LANES), jnp.int32),
                pltpu.VMEM((2, chips, entries, SUBLANES, LANES), dtype),
                pltpu.VMEM((2, chips, groups - 1, entries, SUBLANES, LANES), dtype),
                pltpu.VMEM((groups, chips, sent, SUBLANES, LANES), dtype),
                pltpu.VMEM((groups, chips, sent, SUBLANES, LANES), dtype),
                pltpu.VMEM((chips // BATCHES * (sent + 2), SUBLANES, LANES), jnp.float32),
                pltpu.VMEM((SUBLANES * antennas, samples), dtype),
                pltpu.VMEM((SUBLANES * antennas, samples), dtype),
                pltpu.VMEM((SUBLANES, total_antennas, total_samples), dtype),
                pltpu.VMEM((total_antennas, LANES), jnp.float32),
                pltpu.VMEM((total_antennas, total_antennas), jnp.float32),
                pltpu.SemaphoreType.DMA((4,)),
                pltpu.SemaphoreType.DMA,
                pltpu.SemaphoreType.DMA,
                pltpu.SemaphoreType.DMA((groups, chips)),
                pltpu.SemaphoreType.DMA((groups, BATCHES)),
            ],
            compiler_params=pltpu.CompilerParams(
                collective_id=1 + index, has_side_effects=True, vmem_limit_bytes=48 * 1024 * 1024
            ),
        )

    branches = [unite(index, sent) for index, sent in enumerate(levels)]
    return lax.switch(level[0, 0], branches, first, rest, theirs, table, meta)


def packable(n_chan, n_tm, parts, all_channels, antennas, samples):
    n = n_chan * n_tm
    if n_chan % 2 or n // 2 % (2 * BATCHES) or all_channels % n or SUBLANES % parts:
        return False
    segments = samples // FLAG_BLOCK_WIDTH * antennas
    groups = all_channels // n // (SUBLANES // parts)
    return groups > 1 and all_channels == groups * n * (SUBLANES // parts) and antennas % 16 == 0 and segments * 2 < LANES - 3


def body(n_chan, n_tm, voltages, flag_mask, flagged_prefix_counts):
    chosen = packed_shards if packable(n_chan, n_tm, *voltages.shape) else shards
    return chosen(n_chan, n_tm, voltages, flag_mask, flagged_prefix_counts)


def solution(mesh):
    placed = (P(None, None, "chan", "tm"), P("tm", "chan"), P("tm", "chan"))
    return jax.shard_map(
        functools.partial(body, mesh.shape["chan"], mesh.shape["tm"]),
        mesh=mesh,
        in_specs=placed,
        out_specs=P(("chan", "tm"), None, None, None),
        check_vma=False,
    )
```

```python
import functools

import jax
import jax.numpy as jnp
from jax import lax
from jax.experimental import pallas as pl
from jax.experimental.pallas import tpu as pltpu
from jax.sharding import PartitionSpec as P

FLAG_BLOCK_WIDTH = 128
LANES = 128
SUBLANES = 8
AT, FIRST, LIMIT = 22, 15, 7
BATCHES = 8
LEVEL_STEPS = (16, 22, 25, 26, 27, 28, 29, 30, 31, 32, 33, 34, 42, 64)
MESH = pl.DeviceIdType.MESH
NT = (((1,), (1,)), ((), ()))


def exchange_kernel(
    n_chan, n_tm, groups, volt_ref, limit_ref, out_ref,
    held, table, cols, keep, inverse, send_sem, recv_sem, table_send, table_recv,
):
    n = n_chan * n_tm
    channels = held.shape[1]
    step = channels // groups
    antennas, samples = volt_ref.shape[2], volt_ref.shape[3]
    total_antennas = n_chan * antennas
    local_blocks = samples // FLAG_BLOCK_WIDTH
    my_chan, my_tm = lax.axis_index("chan"), lax.axis_index("tm")
    me = my_chan * n_tm + my_tm

    def swing(m):
        return (m + 1) // 2 * (1 - 2 * lax.rem(m + 1, 2))

    def hop(k):
        return n // 2 + swing(k - 1)

    def place(k):
        other = lax.rem(me + hop(k), n)
        return other, (other // n_tm, lax.rem(other, n_tm))

    barrier = pltpu.get_barrier_semaphore()

    def greet(k, carry):
        pl.semaphore_signal(barrier, inc=1, device_id=place(k)[1], device_id_type=MESH)
        return carry

    lax.fori_loop(1, n, greet, 0)
    pl.semaphore_wait(barrier, n - 1)

    def landing(g):
        return held.at[
            :, pl.ds(g * step, step), my_chan, :, pl.ds(pl.multiple_of(my_tm * samples, LANES), samples)
        ]

    def flag_copy(k):
        return pltpu.make_async_remote_copy(
            src_ref=limit_ref, dst_ref=table.at[me], send_sem=table_send.at[k], recv_sem=table_recv,
            device_id=place(k)[1], device_id_type=MESH,
        )

    def volt_copy(g, k):
        other, where = place(k)
        return pltpu.make_async_remote_copy(
            src_ref=volt_ref.at[:, pl.ds(other * channels + g * step, step)],
            dst_ref=landing(g), send_sem=send_sem.at[g, k], recv_sem=recv_sem.at[g],
            device_id=where, device_id_type=MESH,
        )

    def each(body):
        def run(k, carry):
            body(k)
            return carry

        lax.fori_loop(1, n, run, 0)

    each(lambda k: flag_copy(k).start())
    for g in range(groups):
        each(lambda k, g=g: volt_copy(g, k).start())
    pltpu.make_async_copy(limit_ref, table.at[me], table_recv).start()
    for g in range(groups):
        pltpu.make_async_copy(
            volt_ref.at[:, pl.ds(me * channels + g * step, step)], landing(g), recv_sem.at[g]
        ).start()

    pltpu.make_async_copy(table, table, table_recv).wait()
    rows = table[:, 0, :].astype(jnp.float32)
    padding = -n % LANES
    if padding:
        rows = jnp.concatenate([rows, jnp.zeros((padding, rows.shape[1]), jnp.float32)], axis=0)
    turned = rows.T
    lane = lax.broadcasted_iota(jnp.int32, (total_antennas, LANES), 1).astype(jnp.float32)
    pairs = jnp.zeros((total_antennas, total_antennas), jnp.float32)
    for t in range(n_tm):
        for b in range(local_blocks):
            q = t * local_blocks + b
            for c in range(n_chan):
                source = c * n_tm + t
                cols[c * antennas:(c + 1) * antennas, :] = jnp.broadcast_to(
                    turned[b * antennas:(b + 1) * antennas, source:source + 1], (antennas, LANES)
                )
            column = cols[...]
            keep[:, q * LANES:(q + 1) * LANES] = jnp.where(lane >= column, 1.0, 0.0).astype(keep.dtype)
            pairs += FLAG_BLOCK_WIDTH - jnp.maximum(column[:, :1], column.T[:1, :])
    inverse[...] = 1.0 / jnp.maximum(pairs, 1.0)

    def correlate(c, carry):
        size = (total_antennas, keep.shape[1])
        real = held[0, c].reshape(size) * keep[...]
        imag = held[1, c].reshape(size) * keep[...]
        same = lax.dot_general(real, real, NT, preferred_element_type=jnp.float32)
        same += lax.dot_general(imag, imag, NT, preferred_element_type=jnp.float32)
        cross = lax.dot_general(imag, real, NT, preferred_element_type=jnp.float32)
        out_ref[c, 0] = same * inverse[...]
        out_ref[c, 1] = (cross - cross.T) * inverse[...]
        return carry

    for g in range(groups):
        part = held.at[:, pl.ds(g * step, step)]
        pltpu.make_async_copy(part, part, recv_sem.at[g]).wait()
        lax.fori_loop(g * step, (g + 1) * step, correlate, 0)

    each(lambda k: flag_copy(k).wait_send())
    for g in range(groups):
        each(lambda k, g=g: volt_copy(g, k).wait_send())


def shards(n_chan, n_tm, voltages, flag_mask, flagged_prefix_counts):
    parts, all_channels, antennas, samples = voltages.shape
    n = n_chan * n_tm
    channels = all_channels // n
    total_antennas, total_samples = antennas * n_chan, samples * n_tm
    groups = max(g for g in (4, 2, 1) if channels % g == 0)
    limits = jnp.where(flag_mask == 1, flagged_prefix_counts, FLAG_BLOCK_WIDTH).reshape(1, -1)
    limits = jnp.pad(limits, ((0, 0), (0, -limits.shape[1] % LANES)))
    width = limits.shape[1]
    return pl.pallas_call(
        functools.partial(exchange_kernel, n_chan, n_tm, groups),
        out_shape=pltpu.VMEM((channels, 2, total_antennas, total_antennas), jnp.float32),
        in_specs=[pl.BlockSpec(memory_space=pl.ANY), pl.BlockSpec(memory_space=pltpu.VMEM)],
        out_specs=pl.BlockSpec(memory_space=pltpu.VMEM),
        scratch_shapes=[
            pltpu.VMEM((parts, channels, n_chan, antennas, total_samples), voltages.dtype),
            pltpu.VMEM((n, 1, width), jnp.int32),
            pltpu.VMEM((total_antennas, LANES), jnp.float32),
            pltpu.VMEM((total_antennas, total_samples), voltages.dtype),
            pltpu.VMEM((total_antennas, total_antennas), jnp.float32),
            pltpu.SemaphoreType.DMA((groups, n)),
            pltpu.SemaphoreType.DMA((groups,)),
            pltpu.SemaphoreType.DMA((n,)),
            pltpu.SemaphoreType.DMA,
        ],
        compiler_params=pltpu.CompilerParams(
            collective_id=0, has_side_effects=True, vmem_limit_bytes=48 * 1024 * 1024
        ),
    )(voltages, limits)


def pack_kernel(
    n_chan, n_tm, levels, volt_ref, mask_ref, count_ref, first_ref, rest_ref, theirs_ref, table_ref, meta_ref, level_ref,
    held, theirs, mine, even, odd, row, table, flags, steps,
    load_sem, word_sem, flag_send, flag_recv, pair_send, pair_recv, keep_sem,
):
    n = n_chan * n_tm
    parts, all_channels, antennas, samples = volt_ref.shape
    channels = all_channels // n
    chips, groups = mine.shape[0], mine.shape[1]
    width = SUBLANES // parts
    blocks = samples // FLAG_BLOCK_WIDTH
    segments = blocks * antennas
    my_chan, my_tm = lax.axis_index("chan"), lax.axis_index("tm")
    me = my_chan * n_tm + my_tm
    side = lax.rem(my_chan, 2)
    partner = (my_chan + 1 - 2 * side, my_tm)

    def loop(low, high, do):
        def run(k, carry):
            do(k)
            return carry

        lax.fori_loop(low, high, run, 0)

    def others(do):
        def at(j, low):
            chan = my_chan + j
            chan = jnp.where(chan >= n_chan, chan - n_chan, chan)
            for u in range(low, n_tm):
                t = my_tm + u
                do(j * n_tm + u, (chan, jnp.where(t >= n_tm, t - n_tm, t)))

        loop(1, n_chan, lambda j: at(j, 0))
        at(0, 1)

    barrier = pltpu.get_barrier_semaphore()
    others(lambda k, where: pl.semaphore_signal(barrier, inc=1, device_id=where, device_id_type=MESH))
    words = [pltpu.make_async_copy(ref, flags.at[q], word_sem.at[q]) for q, ref in enumerate((mask_ref, count_ref))]
    for word in words:
        word.start()

    def load(d):
        part = pl.ds(d * channels, channels)
        return pltpu.make_async_copy(volt_ref.at[:, part], held.at[:, part], load_sem.at[d])

    def device_of(j):
        m = lax.rem(j, chips)
        chan = m // n_tm * 2 + lax.rem(side + 1 + j // chips, 2)
        return chan * n_tm + lax.rem(m, n_tm)

    loop(0, n, lambda j: load(device_of(j)).start())
    for word in words:
        word.wait()

    lane = lax.broadcasted_iota(jnp.int32, (SUBLANES, LANES), 1)
    limits = jnp.full((SUBLANES, LANES), FLAG_BLOCK_WIDTH, jnp.int32)
    total = jnp.int32(0)
    for s in range(segments):
        b, i = s // antennas, s % antennas
        flags[1, b, i] = jnp.where(flags[0, b, i] == 1, flags[1, b, i], FLAG_BLOCK_WIDTH)
        total = total + FLAG_BLOCK_WIDTH - flags[1, b, i]
    start = side * ((-total) & (LANES - 1))
    for s in range(segments):
        b, i = s // antennas, s % antennas
        limit = flags[1, b, i]
        limits = jnp.where(lane == s, limit, limits)
        first = start & (LANES - 1)
        spills = first + FLAG_BLOCK_WIDTH - limit > LANES
        steps[0, s] = (first - limit) & (LANES - 1)
        steps[1, s] = first
        steps[2, s] = jnp.where(spills, 0, first)
        start = start + FLAG_BLOCK_WIDTH - limit
    row[...] = limits[:1]

    old = lax.broadcasted_iota(jnp.int32, (SUBLANES * antennas, SUBLANES * antennas), 1)
    new = lax.broadcasted_iota(jnp.int32, (SUBLANES * antennas, SUBLANES * antennas), 0)
    turn = jnp.where(old == lax.rem(new, SUBLANES) * antennas + new // SUBLANES, 1.0, 0.0).astype(volt_ref.dtype)

    def flatten(j, flat):
        d = device_of(j)
        load(d).wait()
        for g in range(groups):
            part = held[:, pl.ds(d * channels + g * width, width)].reshape(SUBLANES * antennas, samples)
            flat[g] = jnp.dot(turn, part, preferred_element_type=jnp.float32)

    def merge(flat, target, m):
        carry = [jnp.zeros((SUBLANES, LANES), jnp.float32)] * groups
        for s in range(segments):
            b, i = s // antennas, s % antennas
            shift, opens, stays = steps[0, s], lane >= steps[1, s], lane >= steps[2, s]
            for g in range(groups):
                piece = flat[g, i * SUBLANES:(i + 1) * SUBLANES, b * LANES:(b + 1) * LANES]
                piece = pltpu.roll(piece, shift, axis=1)
                target[m, g, s] = jnp.where(opens, piece, carry[g]).astype(target.dtype)
                carry[g] = jnp.where(stays, piece, carry[g])
        for g in range(groups):
            target[m, g, segments] = carry[g].astype(target.dtype)

    def flag_copy(k, where):
        return pltpu.make_async_remote_copy(
            src_ref=row, dst_ref=table.at[me], send_sem=flag_send.at[k], recv_sem=flag_recv,
            device_id=where, device_id_type=MESH,
        )

    pair_copy = pltpu.make_async_remote_copy(
        src_ref=theirs.at[:, 0], dst_ref=first_ref.at[1], send_sem=pair_send, recv_sem=pair_recv,
        device_id=partner, device_id_type=MESH,
    )

    def keeps(h):
        part, later = pl.ds(2 * h, 2), pl.ds(1, groups - 1)
        return [
            pltpu.make_async_copy(ref, where, keep_sem.at[q, h])
            for q, (ref, where) in enumerate((
                (theirs.at[part, later], theirs_ref.at[part]),
                (mine.at[part, 0], first_ref.at[0, part]),
                (mine.at[part, later], rest_ref.at[part]),
            ))
        ]

    def keep_mine(h):
        for keep in keeps(h)[1:]:
            keep.start()

    def wait_keeps(h):
        for keep in keeps(h):
            keep.wait()

    def pack_theirs(h):
        flatten(2 * h + 1, odd)
        merge(even, theirs, 2 * h)
        flatten(2 * h + 2, even)
        merge(odd, theirs, 2 * h + 1)
        keeps(h)[0].start()

    def pack_mine(h):
        flatten(chips + 2 * h + 1, odd)
        merge(even, mine, 2 * h)
        flatten(chips + 2 * h + 2, even)
        merge(odd, mine, 2 * h + 1)
        keep_mine(h)

    flatten(0, even)
    early = chips * 5 // 16
    loop(0, early, pack_theirs)
    pl.semaphore_wait(barrier, n - 1)
    others(lambda k, where: flag_copy(k, where).start())
    loop(early, chips // 2, pack_theirs)
    pair_copy.start()
    pltpu.make_async_copy(row, table.at[me], flag_recv).start()
    loop(0, chips // 2 - 1, pack_mine)
    flatten(n - 1, odd)
    merge(even, mine, chips - 2)
    merge(odd, mine, chips - 1)
    keep_mine(chips // 2 - 1)

    pltpu.make_async_copy(table, table, flag_recv).wait()
    rows = table[:, 0, :]
    lanes = lax.broadcasted_iota(jnp.int32, (n, LANES), 1)
    kept = (FLAG_BLOCK_WIDTH - rows).astype(jnp.float32).astype(jnp.bfloat16)
    above = jnp.where(
        lax.broadcasted_iota(jnp.int32, (LANES, LANES), 0) < lax.broadcasted_iota(jnp.int32, (LANES, LANES), 1), 1.0, 0.0
    ).astype(jnp.bfloat16)
    offset = jnp.dot(kept, above, preferred_element_type=jnp.float32).astype(jnp.int32)
    total = jnp.broadcast_to(jnp.max(offset, axis=1, keepdims=True), (n, LANES))
    full = (total + (LANES - 1)) >> 7
    second = lax.rem(lax.broadcasted_iota(jnp.int32, (n, LANES), 0) // n_tm, 2) == 1
    offset = offset + jnp.where(second, (-total) & (LANES - 1), 0)
    to = lax.broadcasted_iota(jnp.int32, (n, n), 0)
    frm = lax.broadcasted_iota(jnp.int32, (n, n), 1)
    behind = jnp.where((frm == to - n_tm) & (lax.rem(to // n_tm, 2) == 1), 1.0, 0.0).astype(jnp.bfloat16)

    def fetch_behind(x):
        x = x.astype(jnp.float32).astype(jnp.bfloat16)
        return jnp.dot(behind, x, preferred_element_type=jnp.float32).astype(jnp.int32)

    ahead = (fetch_behind(total >> 7) << 7) + fetch_behind(total & (LANES - 1))
    pair = (total + ahead + (LANES - 1)) >> 7
    base = jnp.where(second, pair - full, 0)
    at = offset >> 7
    first = offset & (LANES - 1)
    meta_ref[0] = ((base + at) << AT) | (first << FIRST) | (rows << LIMIT) | ((rows - first) & (LANES - 1))
    place_of = jnp.full((n, LANES), -1, jnp.int32)
    for s in range(segments + 1):
        place_of += jnp.where(at[:, s:s + 1] <= lanes, 1, 0)
    place_of = jnp.where(lanes == LANES - 1, full, place_of)
    place_of = jnp.where(lanes == LANES - 2, base, place_of)
    meta_ref[1] = jnp.where(lanes == LANES - 3, total & (LANES - 1), place_of)
    table_ref[...] = rows
    need = jnp.max(pair, axis=0, keepdims=True)
    level = jnp.zeros((1, LANES), jnp.int32)
    for q in levels[:-1]:
        level += jnp.where(need > q, 1, 0)
    level_ref[...] = level

    loop(0, chips // 2, wait_keeps)
    pair_copy.wait()
    others(lambda k, where: flag_copy(k, where).wait_send())


def unite_kernel(
    n_chan, n_tm, antennas, samples, sent, first_ref, rest_ref, theirs_ref, table_hbm, meta_hbm, out_ref,
    table_ref, meta_ref, first, rest, ready, landing, work, even, odd, square, cols, inverse,
    fetch_sem, pair_send, pair_recv, send_sem, recv_sem,
):
    groups = landing.shape[0]
    n, chips = n_chan * n_tm, first_ref.shape[1]
    half, batch = chips // 2, chips // recv_sem.shape[1]
    total_antennas, total_samples = square.shape[1], square.shape[2]
    blocks = samples // FLAG_BLOCK_WIDTH
    channels = out_ref.shape[0]
    width = channels // groups
    my_chan, my_tm = lax.axis_index("chan"), lax.axis_index("tm")
    side = lax.rem(my_chan, 2)
    here = my_chan // 2 * n_tm + my_tm
    my_half, my_place = here // half, lax.rem(here, half)
    partner = (my_chan + 1 - 2 * side, my_tm)

    def loop(low, high, do):
        def run(k, carry):
            do(k)
            return carry

        lax.fori_loop(low, high, run, 0)

    def chip_at(slot, step):
        other_half = lax.rem(my_half + slot // half, 2)
        return other_half * half + lax.rem(my_place + half + step * lax.rem(slot, half), half)

    def device_at(chip):
        return (chip // n_tm * 2 + side, lax.rem(chip, n_tm))

    barrier = pltpu.get_barrier_semaphore()
    loop(1, chips, lambda k: pl.semaphore_signal(
        barrier, inc=1, device_id=device_at(lax.rem(here + k, chips)), device_id_type=MESH
    ))
    pl.semaphore_signal(barrier, inc=1, device_id=partner, device_id_type=MESH)
    fetches = [
        pltpu.make_async_copy(first_ref, first, fetch_sem.at[0]),
        pltpu.make_async_copy(rest_ref, rest.at[0], fetch_sem.at[1]),
        pltpu.make_async_copy(meta_hbm, meta_ref, fetch_sem.at[2]),
        pltpu.make_async_copy(table_hbm, table_ref, fetch_sem.at[3]),
    ]
    for q in (2, 0, 3, 1):
        fetches[q].start()
    pair_copy = pltpu.make_async_remote_copy(
        src_ref=theirs_ref, dst_ref=rest.at[1], send_sem=pair_send, recv_sem=pair_recv,
        device_id=partner, device_id_type=MESH,
    )
    fetches[2].wait()
    low_device = (my_chan - side) * n_tm + my_tm
    high_device = low_device + n_tm
    low_rows, low_fill = meta_ref[1, low_device, LANES - 1], meta_ref[1, low_device, LANES - 3]
    high_base = meta_ref[1, high_device, LANES - 2]
    lanes = lax.broadcasted_iota(jnp.int32, (chips, SUBLANES, LANES), 2)

    def gather(g, source):
        def pick(r):
            low = source(side, meta_ref[1, low_device, r]).astype(jnp.float32)
            high = source(1 - side, meta_ref[1, high_device, jnp.maximum(r - high_base, 0)]).astype(jnp.float32)
            bound = jnp.where(r < high_base, LANES, jnp.where(r < low_rows, low_fill, 0))
            ready[g, :, r] = jnp.where(lanes < bound, low, high).astype(ready.dtype)

        loop(0, sent, pick)

    def copy(g, slot):
        chip = chip_at(slot, 1)
        return pltpu.make_async_remote_copy(
            src_ref=ready.at[g, chip], dst_ref=landing.at[g, slot, pl.ds(0, sent)],
            send_sem=send_sem.at[g, slot], recv_sem=recv_sem.at[g, slot // batch],
            device_id=device_at(chip), device_id_type=MESH,
        )

    def launch(g):
        loop(1, half, lambda slot: copy(g, slot).start())
        loop(0, half, lambda slot: copy(g, half + lax.rem(slot + side * (half // 2), half)).start())
        pltpu.make_async_copy(ready.at[g, here], landing.at[g, 0, pl.ds(0, sent)], recv_sem.at[g, 0]).start()

    def gather_and_launch(g):
        gather(g, lambda w, entry: rest[w, :, g - 1, entry])
        launch(g)

    fetches[0].wait()
    gather(0, lambda w, entry: first[w, :, entry])
    pl.semaphore_wait(barrier, chips)
    pair_copy.start()
    launch(0)
    fetches[1].wait()
    pair_copy.wait_recv()
    loop(1, groups, gather_and_launch)

    fetches[3].wait()
    rows = table_ref[...].astype(jnp.float32)
    padding = -n % LANES
    if padding:
        rows = jnp.concatenate([rows, jnp.zeros((padding, rows.shape[1]), jnp.float32)], axis=0)
    turned = rows.T
    pairs = jnp.zeros((total_antennas, total_antennas), jnp.float32)
    for t in range(n_tm):
        for b in range(blocks):
            for c in range(n_chan):
                source = c * n_tm + t
                cols[c * antennas:(c + 1) * antennas, :] = jnp.broadcast_to(
                    turned[b * antennas:(b + 1) * antennas, source:source + 1], (antennas, LANES)
                )
            column = cols[...]
            pairs += FLAG_BLOCK_WIDTH - jnp.maximum(column[:, :1], column.T[:1, :])
    inverse[...] = 1.0 / jnp.maximum(pairs, 1.0)

    lane = lax.broadcasted_iota(jnp.int32, (SUBLANES, LANES), 1)
    old = lax.broadcasted_iota(jnp.int32, (SUBLANES * antennas, SUBLANES * antennas), 1)
    new = lax.broadcasted_iota(jnp.int32, (SUBLANES * antennas, SUBLANES * antennas), 0)
    turn = jnp.where(new == lax.rem(old, SUBLANES) * antennas + old // SUBLANES, 1.0, 0.0).astype(square.dtype)

    lane_first = (lane << FIRST) | ((1 << FIRST) - 1)
    lane_limit = (lane << LIMIT) | ((1 << LIMIT) - 1)
    first_bits, limit_bits = (1 << AT) - (1 << FIRST), (1 << FIRST) - (1 << LIMIT)

    def source(part, q):
        chip = chip_at(part * batch + q // 2, -1)
        return chip // n_tm * 2 + lax.rem(q, 2), lax.rem(chip, n_tm)

    def expand(part, q, z):
        q = jnp.minimum(q, 2 * batch - 1)
        chan, t = source(part, q)
        d = chan * n_tm + t
        origin = q // 2 * (sent + 2)
        for i in range(antennas):
            for b in range(blocks):
                word = meta_ref[0, d, b * antennas + i]
                at = origin + (word >> AT)
                spread = jnp.full(lane.shape, word, jnp.int32)
                piece = jnp.where((spread & first_bits) <= lane_first, work[at], work[at + 1])
                piece = pltpu.roll(piece, word, axis=1)
                piece = jnp.where((spread & limit_bits) <= lane_limit, piece, 0.0)
                z[i * SUBLANES:(i + 1) * SUBLANES, b * LANES:(b + 1) * LANES] = piece.astype(z.dtype)

    def settle(part, q, z):
        chan, t = source(part, q)
        flat = jnp.dot(turn, z[...], preferred_element_type=jnp.float32).astype(square.dtype)
        for p in range(SUBLANES):
            square[
                p, pl.ds(pl.multiple_of(chan * antennas, antennas), antennas),
                pl.ds(pl.multiple_of(t * samples, LANES), samples),
            ] = flat[p * antennas:(p + 1) * antennas]

    def receive(g, part):
        arrived = landing.at[g, pl.ds(part * batch, batch), pl.ds(0, sent)]
        pltpu.make_async_copy(arrived, arrived, recv_sem.at[g, part]).wait()
        for j in range(batch):
            work[j * (sent + 2):j * (sent + 2) + sent] = landing[g, part * batch + j, :sent].astype(jnp.float32)
        expand(part, 0, even)

        def two(h):
            expand(part, 2 * h + 1, odd)
            settle(part, 2 * h, even)
            expand(part, 2 * h + 2, even)
            settle(part, 2 * h + 1, odd)

        loop(0, batch, two)

    def finish(g):
        loop(0, chips // batch, lambda part: receive(g, part))

        def correlate(c):
            real, imag = square[c], square[width + c]
            same = lax.dot_general(real, real, NT, preferred_element_type=jnp.float32)
            same += lax.dot_general(imag, imag, NT, preferred_element_type=jnp.float32)
            cross = lax.dot_general(imag, real, NT, preferred_element_type=jnp.float32)
            channel = g * width + c
            out_ref[channel, 0] = same * inverse[...]
            out_ref[channel, 1] = (cross - cross.T) * inverse[...]

        loop(0, width, correlate)

    loop(0, groups, finish)
    pair_copy.wait_send()
    loop(0, groups, lambda g: loop(1, chips, lambda slot: copy(g, slot).wait_send()))


def packed_shards(n_chan, n_tm, voltages, flag_mask, flagged_prefix_counts):
    parts, all_channels, antennas, samples = voltages.shape
    n = n_chan * n_tm
    chips = n // 2
    channels = all_channels // n
    width = SUBLANES // parts
    groups = channels // width
    blocks = samples // FLAG_BLOCK_WIDTH
    segments = blocks * antennas
    most = 2 * segments
    levels = tuple(sorted({-(-most * step // LEVEL_STEPS[-1]) for step in LEVEL_STEPS}))
    dtype = voltages.dtype
    entries = segments + 1
    vmem = pl.BlockSpec(memory_space=pltpu.VMEM)
    hbm = pl.BlockSpec(memory_space=pltpu.HBM)
    first, rest, theirs, table, meta, level = pl.pallas_call(
        functools.partial(pack_kernel, n_chan, n_tm, levels),
        out_shape=(
            jax.ShapeDtypeStruct((2, chips, entries, SUBLANES, LANES), dtype),
            jax.ShapeDtypeStruct((chips, groups - 1, entries, SUBLANES, LANES), dtype),
            jax.ShapeDtypeStruct((chips, groups - 1, entries, SUBLANES, LANES), dtype),
            jax.ShapeDtypeStruct((n, LANES), jnp.int32),
            jax.ShapeDtypeStruct((2, n, LANES), jnp.int32),
            jax.ShapeDtypeStruct((1, LANES), jnp.int32),
        ),
        in_specs=[hbm, hbm, hbm],
        out_specs=(hbm, hbm, hbm, vmem, vmem, vmem),
        scratch_shapes=[
            pltpu.VMEM(voltages.shape, dtype),
            pltpu.VMEM((chips, groups, entries, SUBLANES, LANES), dtype),
            pltpu.VMEM((chips, groups, entries, SUBLANES, LANES), dtype),
            pltpu.VMEM((groups, SUBLANES * antennas, samples), jnp.float32),
            pltpu.VMEM((groups, SUBLANES * antennas, samples), jnp.float32),
            pltpu.VMEM((1, LANES), jnp.int32),
            pltpu.VMEM((n, 1, LANES), jnp.int32),
            pltpu.SMEM((2,) + flag_mask.shape, jnp.int32),
            pltpu.SMEM((3, segments), jnp.int32),
            pltpu.SemaphoreType.DMA((n,)),
            pltpu.SemaphoreType.DMA((2,)),
            pltpu.SemaphoreType.DMA((n,)),
            pltpu.SemaphoreType.DMA,
            pltpu.SemaphoreType.DMA,
            pltpu.SemaphoreType.DMA,
            pltpu.SemaphoreType.DMA((3, chips // 2)),
        ],
        compiler_params=pltpu.CompilerParams(
            collective_id=0, has_side_effects=True, vmem_limit_bytes=67043328
        ),
    )(voltages, flag_mask, flagged_prefix_counts)
    total_antennas, total_samples = antennas * n_chan, samples * n_tm

    def unite(index, sent):
        return pl.pallas_call(
            functools.partial(unite_kernel, n_chan, n_tm, antennas, samples, sent),
            out_shape=pltpu.VMEM((channels, 2, total_antennas, total_antennas), jnp.float32),
            in_specs=[hbm] * 5,
            out_specs=vmem,
            scratch_shapes=[
                pltpu.VMEM((n, LANES), jnp.int32),
                pltpu.SMEM((2, n, LANES), jnp.int32),
                pltpu.VMEM((2, chips, entries, SUBLANES, LANES), dtype),
                pltpu.VMEM((2, chips, groups - 1, entries, SUBLANES, LANES), dtype),
                pltpu.VMEM((groups, chips, sent, SUBLANES, LANES), dtype),
                pltpu.VMEM((groups, chips, sent, SUBLANES, LANES), dtype),
                pltpu.VMEM((chips // BATCHES * (sent + 2), SUBLANES, LANES), jnp.float32),
                pltpu.VMEM((SUBLANES * antennas, samples), dtype),
                pltpu.VMEM((SUBLANES * antennas, samples), dtype),
                pltpu.VMEM((SUBLANES, total_antennas, total_samples), dtype),
                pltpu.VMEM((total_antennas, LANES), jnp.float32),
                pltpu.VMEM((total_antennas, total_antennas), jnp.float32),
                pltpu.SemaphoreType.DMA((4,)),
                pltpu.SemaphoreType.DMA,
                pltpu.SemaphoreType.DMA,
                pltpu.SemaphoreType.DMA((groups, chips)),
                pltpu.SemaphoreType.DMA((groups, BATCHES)),
            ],
            compiler_params=pltpu.CompilerParams(
                collective_id=1 + index, has_side_effects=True, vmem_limit_bytes=48 * 1024 * 1024
            ),
        )

    branches = [unite(index, sent) for index, sent in enumerate(levels)]
    return lax.switch(level[0, 0], branches, first, rest, theirs, table, meta)


def packable(n_chan, n_tm, parts, all_channels, antennas, samples):
    n = n_chan * n_tm
    if n_chan % 2 or n // 2 % (2 * BATCHES) or all_channels % n or SUBLANES % parts:
        return False
    segments = samples // FLAG_BLOCK_WIDTH * antennas
    groups = all_channels // n // (SUBLANES // parts)
    return groups > 1 and all_channels == groups * n * (SUBLANES // parts) and antennas % 16 == 0 and segments * 2 < LANES - 3


def body(n_chan, n_tm, voltages, flag_mask, flagged_prefix_counts):
    chosen = packed_shards if packable(n_chan, n_tm, *voltages.shape) else shards
    return chosen(n_chan, n_tm, voltages, flag_mask, flagged_prefix_counts)


def solution(mesh):
    placed = (P(None, None, "chan", "tm"), P("tm", "chan"), P("tm", "chan"))
    return jax.shard_map(
        functools.partial(body, mesh.shape["chan"], mesh.shape["tm"]),
        mesh=mesh,
        in_specs=placed,
        out_specs=P(("chan", "tm"), None, None, None),
        check_vma=False,
    )
```
